128 devices in a mesh: rep: 2 (over core), dp: 64 (over x, y, z).
Axes of the slice: x: 4, y: 4, z: 4, core: 2. Of those that a mesh axis runs over, the one named last changes fastest.
Arguments:
- x: bfloat16 [128, 2048, 768], P(('rep', 'dp')), parts along dimension 0
- dy: bfloat16 [128, 2048, 768], P(('rep', 'dp')), parts along dimension 0
- w_gate: bfloat16 [2, 768, 3072], replicated
- w_up: bfloat16 [2, 768, 3072], replicated
- w_down: bfloat16 [2, 3072, 768], replicated
- m_w_gate: float32 [2, 768, 3072], P(None, 'dp')
- m_w_up: float32 [2, 768, 3072], P(None, 'dp')
- m_w_down: float32 [2, 3072, 768], P(None, 'dp')
- v_w_gate: float32 [2, 768, 3072], P(None, 'dp')
- v_w_up: float32 [2, 768, 3072], P(None, 'dp')
- v_w_down: float32 [2, 3072, 768], P(None, 'dp')
Outputs:
- output 1: bfloat16 [4, 768, 3072], P('rep'), parts along dimension 0
- output 2: bfloat16 [4, 768, 3072], P('rep'), parts along dimension 0
- output 3: bfloat16 [4, 3072, 768], P('rep'), parts along dimension 0
- output 4: float32 [4, 768, 3072], P('rep', 'dp'), parts along dimension 0
- output 5: float32 [4, 768, 3072], P('rep', 'dp'), parts along dimension 0
- output 6: float32 [4, 3072, 768], P('rep', 'dp'), parts along dimension 0
- output 7: float32 [4, 768, 3072], P('rep', 'dp'), parts along dimension 0
- output 8: float32 [4, 768, 3072], P('rep', 'dp'), parts along dimension 0
- output 9: float32 [4, 3072, 768], P('rep', 'dp'), parts along dimension 0
There are 2 independent parts. The reference program is written for one: setup_inputs(seed, part) draws one part's arguments, and reference() takes and returns one part's arrays. A program takes and returns all parts, laid end to end along the dimension named above; an argument that names none is the same for every part.
All inputs are finite; a program needn't handle non-finite values.
Results may differ from the reference program's by a relative error of at most 0.022.
Values are sent between devices in bfloat16 or wider.
A program may use at most 1.5 GiB of HBM per device.

```python
import jax
import jax.numpy as jnp
from jax import lax

SEQUENCES = 64
TOKENS = 2048
D = 768
FF = 3072
LAYERS = 2
NAMES = ("w_gate", "w_up", "w_down")
SHAPES = {"w_gate": (LAYERS, D, FF), "w_up": (LAYERS, D, FF), "w_down": (LAYERS, FF, D)}


def bump(key, n, height):
    away = (jnp.arange(n, dtype=jnp.int32) - jax.random.randint(key, (), 0, n, jnp.int32)) % n
    return jnp.where(away < n // 8, height, 1.0)


def together(key, own, strength):
    shared = jax.random.normal(key, own.shape[1:], jnp.float32)
    return (own + strength * shared) * lax.rsqrt(1 + strength * strength)


def setup_inputs(seed: int = 0, part: int = 0) -> dict:
    kx, kdy, ka, kb, kz, kf, kh, kl, *keys = jax.random.split(jax.random.key(seed), 8 + 3 * len(NAMES))
    kx, kdy, ka, kb = (jax.random.fold_in(k, part) for k in (kx, kdy, ka, kb))
    kw, km, kv = (keys[i::3] for i in range(3))
    shape = (SEQUENCES, TOKENS, D)
    much_x, much_dy = jax.random.uniform(kz, (2,), jnp.float32, 0.0, 1.0)
    loud = 2.0 ** jax.random.uniform(jax.random.fold_in(kz, 1), (), jnp.float32, -1.0, 2.0)
    layers = 2.0 ** jax.random.uniform(kl, (LAYERS, 1, 1), jnp.float32, -1.0, 1.0)
    x = together(ka, jax.random.normal(kx, shape, jnp.float32), much_x) * bump(kf, D, 4.0)
    dy = together(kb, jax.random.normal(kdy, shape, jnp.float32), much_dy)
    drawn = {"x": x.astype(jnp.bfloat16), "dy": (loud * dy * (SEQUENCES * TOKENS) ** -0.5).astype(jnp.bfloat16)}
    for key, name in zip(kw, NAMES, strict=True):
        w = jax.random.normal(key, SHAPES[name], jnp.float32) * SHAPES[name][1] ** -0.5
        drawn[name] = (w * {"w_gate": 1.0, "w_up": bump(kh, FF, 4.0), "w_down": layers}[name]).astype(jnp.bfloat16)
    for key, name in zip(km, NAMES, strict=True):
        drawn[f"m_{name}"] = 0.1 * jax.random.normal(key, SHAPES[name], jnp.float32)
    for key, name in zip(kv, NAMES, strict=True):
        drawn[f"v_{name}"] = loud * loud * jax.random.uniform(key, SHAPES[name], jnp.float32, 0.05, 0.15)
    return drawn


def matmul(a, w):
    return jnp.dot(a, w, preferred_element_type=jnp.float32).astype(jnp.bfloat16)


def normed(h):
    wide = h.astype(jnp.float32)
    scale = lax.rsqrt(jnp.mean(wide**2, -1, keepdims=True) + 1e-6)
    return (wide * scale).astype(jnp.bfloat16)


def layer(h, w):
    a = normed(h)
    gate = jnp.dot(a, w["w_gate"], preferred_element_type=jnp.float32)
    up = jnp.dot(a, w["w_up"], preferred_element_type=jnp.float32)
    return h + matmul((jax.nn.silu(gate) * up).astype(jnp.bfloat16), w["w_down"])


def adamw(w, m, v, g):
    m = 0.9 * m + 0.1 * g
    v = 0.95 * v + 0.05 * g * g
    step = m * lax.rsqrt(v + 1e-8) + 0.1 * w
    return (w - 0.02 * step).astype(jnp.bfloat16), m, v


def stack(weights, h):
    return lax.scan(lambda h, w: (layer(h, w), None), h, weights)[0]


def reference(x, dy, w_gate, w_up, w_down, m_w_gate, m_w_up, m_w_down, v_w_gate, v_w_up, v_w_down):
    weights = dict(zip(NAMES, (w_gate, w_up, w_down), strict=True))

    def take(so_far, sequence):
        h, by_y = sequence
        _, back = jax.vjp(lambda w: stack(w, h), weights)
        return jax.tree.map(lambda total, term: total + term.astype(jnp.float32), so_far, back(by_y)[0]), None

    none_yet = {name: jnp.zeros(w.shape, jnp.float32) for name, w in weights.items()}
    by_weights, _ = lax.scan(take, none_yet, (x, dy))
    gradients = [by_weights[name].astype(jnp.bfloat16).astype(jnp.float32) for name in NAMES]
    new = [
        adamw(w.astype(jnp.float32), m, v, g)
        for w, m, v, g in zip((w_gate, w_up, w_down), (m_w_gate, m_w_up, m_w_down), (v_w_gate, v_w_up, v_w_down), gradients, strict=True)
    ]
    return tuple(one[which] for which in range(3) for one in new)
```

```python
import functools

import jax
import jax.numpy as jnp
from jax import lax
from jax.experimental import pallas as pl
from jax.experimental.pallas import tpu as pltpu
from jax.sharding import PartitionSpec as P

F32 = jnp.float32
BF16 = jnp.bfloat16
MESH = pl.DeviceIdType.MESH
ANY = pl.BlockSpec(memory_space=pl.ANY)
VMEM = pl.BlockSpec(memory_space=pltpu.VMEM)
STRIDE = (16, 4, 1)
ORDER = ((0, 1, 2), (1, 2, 0), (2, 0, 1))
VMEM_LIMIT = 60 * 1024 * 1024


def matmul(a, w):
    return jnp.dot(a, w, preferred_element_type=F32).astype(BF16)


def over_tokens(a, b):
    return lax.dot_general(a, b, (((0,), (0,)), ((), ())), preferred_element_type=F32)


def wide_kernel(a_ref, d_ref, out_ref, s_ref):
    s_ref[...] = over_tokens(a_ref[...], d_ref[...])

    def two_devices(i, _):
        rows = s_ref[pl.ds(pl.multiple_of(24 * i, 8), 24), :]
        for k in range(2):
            block = [rows[12 * k : 12 * k + 12, 128 * q : 128 * q + 128] for q in range(4)]
            out_ref[0, 2 * i + k] = jnp.concatenate(block, axis=0).astype(BF16)
        return 0

    lax.fori_loop(0, 32, two_devices, 0)


def wide_gradient(a, d):
    tokens, rows = a.shape
    return pl.pallas_call(
        wide_kernel,
        grid=(6,),
        in_specs=[pl.BlockSpec((tokens, rows), lambda j: (0, 0)), pl.BlockSpec((tokens, 512), lambda j: (0, j))],
        out_specs=pl.BlockSpec((1, 64, 48, 128), lambda j: (j, 0, 0, 0)),
        out_shape=jax.ShapeDtypeStruct((6, 64, 48, 128), BF16),
        scratch_shapes=[pltpu.VMEM((rows, 512), F32)],
        compiler_params=pltpu.CompilerParams(vmem_limit_bytes=VMEM_LIMIT),
        cost_estimate=pl.CostEstimate(flops=2 * tokens * rows * 3072, bytes_accessed=20 << 20, transcendentals=0),
    )(a, d)


def down_kernel(act_ref, d_ref, out_ref):
    total = over_tokens(act_ref[...], d_ref[...])
    for j in range(6):
        out_ref[j] = total[:, 128 * j : 128 * j + 128].astype(BF16)


def down_gradient(act, d):
    tokens, columns = d.shape
    out = pl.pallas_call(
        down_kernel,
        grid=(6,),
        in_specs=[pl.BlockSpec((tokens, 512), lambda i: (0, i)), pl.BlockSpec((tokens, columns), lambda i: (0, 0))],
        out_specs=pl.BlockSpec((6, 512, 128), lambda i: (0, i, 0)),
        out_shape=jax.ShapeDtypeStruct((6, 3072, 128), BF16),
        compiler_params=pltpu.CompilerParams(vmem_limit_bytes=VMEM_LIMIT),
        cost_estimate=pl.CostEstimate(flops=2 * tokens * columns * 3072, bytes_accessed=20 << 20, transcendentals=0),
    )(act, d)
    return out.reshape(6, 64, 48, 128)


def adamw(w, m, v, g):
    m = 0.9 * m + 0.1 * g
    v = 0.95 * v + 0.05 * g * g
    step = m * lax.rsqrt(v + 1e-8) + 0.1 * w
    return w - 0.02 * step, m, v


class Exchange:
    def __init__(self, number, g_refs, w_refs, m_refs, v_refs, sum_ref, full_ref, out_ref, bufs, own, scratch, sems):
        self.number, self.g, self.w, self.m, self.v = number, g_refs, w_refs, m_refs, v_refs
        self.sum, self.full, self.out, self.bufs, self.own, self.scratch = sum_ref, full_ref, out_ref, bufs, own, scratch
        self.send_sem, self.recv_sem, self.own_sem, self.out_sem = sems
        me = lax.axis_index("dp")
        self.at = (me // 16, (me // 4) % 4, me % 4)
        self.right = tuple(me + STRIDE[a] * ((self.at[a] + 1) % 4 - self.at[a]) for a in range(3))
        self.left = tuple(me + STRIDE[a] * ((self.at[a] + 3) % 4 - self.at[a]) for a in range(3))

    def barrier(self):
        barrier = pltpu.get_barrier_semaphore()
        for axis in range(3):
            for to in (self.left[axis], self.right[axis]):
                pl.semaphore_signal(barrier, inc=1, device_id={"dp": to}, device_id_type=MESH)
        pl.semaphore_wait(barrier, 6)

    def copy(self, key, src, dst, to):
        m, c, phase, which = key
        n = 6 * phase + which
        return pltpu.make_async_remote_copy(
            src_ref=src,
            dst_ref=dst,
            send_sem=self.send_sem.at[3 * m + c, n],
            recv_sem=self.recv_sem.at[3 * m + c, n],
            device_id={"dp": to},
            device_id_type=MESH,
        )

    def block(self, m, c, phase, half, k):
        axis = ORDER[c][phase]
        place = sorted(ORDER[c][phase:]).index(axis)
        where = (slice(None),) * place + (k,)
        if phase == 0:
            return self.g[m].at[(2 * c + half, *where)]
        return self.bufs[phase - 1][1].at[(m, c, half, *where)]

    def reduce_copies(self, m, c, phase):
        axis = ORDER[c][phase]
        p, left, right = self.at[axis], self.left[axis], self.right[axis]
        one, of_left, of_right = (b.at[m, c] for b in self.bufs[phase])
        after, before, across = (p + 1) % 4, (p + 3) % 4, (p + 2) % 4
        block = functools.partial(self.block, m, c, phase)
        parts = (
            (block(0, across), one.at[0], right),
            (block(1, across), one.at[1], left),
            (block(1, after), of_left.at[1], right),
            (block(0, before), of_right.at[0], left),
            (one.at[0], of_left.at[0], right),
            (one.at[1], of_right.at[1], left),
        )
        return [functools.partial(self.copy, (m, c, phase, i), *part) for i, part in enumerate(parts)]

    def own_copies(self, m, c):
        p = self.at[ORDER[c][0]]
        blocks = ((0, (p + 1) % 4), (1, (p + 3) % 4), (0, p), (1, p))
        return [
            functools.partial(pltpu.make_async_copy, self.block(m, c, 0, *b), self.own.at[m, c, i], self.own_sem.at[3 * m + c, i])
            for i, b in enumerate(blocks)
        ]

    def add(self, phase, into, *others):
        def total(where):
            t = into[where].astype(F32)
            for o in others:
                t += o[where].astype(F32)
            into[where] = t.astype(BF16)

        if phase == 2:
            total(Ellipsis)
        elif phase == 1:
            for i in range(4):
                total((i,))
        else:

            def some(i, _):
                for k in range(4):
                    total((i, k))
                return 0

            lax.fori_loop(0, 4, some, 0)

    def begin(self, m, c, phase):
        for copy in self.reduce_copies(m, c, phase)[:4]:
            copy().start()
        if phase == 0:
            for copy in self.own_copies(m, c):
                copy().start()

    def pass_on(self, m, c, phase):
        copies = self.reduce_copies(m, c, phase)
        p = self.at[ORDER[c][phase]]
        one = self.bufs[phase][0].at[m, c]
        mine = self.own_copies(m, c) if phase == 0 else None
        for half, k in ((0, (p + 1) % 4), (1, (p + 3) % 4)):
            if phase == 0:
                mine[half]().wait()
            copies[half]().wait_recv()
            self.add(phase, one.at[half], self.own.at[m, c, half] if phase == 0 else self.block(m, c, phase, half, k))
            copies[4 + half]().start()

    def finish(self, m, c, phase):
        copies = self.reduce_copies(m, c, phase)
        p = self.at[ORDER[c][phase]]
        _, of_left, of_right = (b.at[m, c] for b in self.bufs[phase])
        mine = self.own_copies(m, c) if phase == 0 else None
        for half in range(2):
            if phase == 0:
                mine[2 + half]().wait()
            here = self.own.at[m, c, 2 + half] if phase == 0 else self.block(m, c, phase, half, p)
            for i in ((4, 3), (2, 5))[half]:
                copies[i]().wait_recv()
            if phase < 2:
                self.add(phase, of_left.at[half], of_right.at[half], here)
            else:
                self.update(m, 2 * c + half, of_left[half].astype(F32) + of_right[half].astype(F32) + here[...].astype(F32))

    def update(self, m, j, g):
        g = g.astype(BF16).astype(F32)
        self.sum[m, j] = g
        x, y, z = self.at
        n = self.number
        if m == 0:
            where = (n, slice(None), pl.ds(128 * j, 128))
            new = adamw(self.w[m][where].astype(F32), self.m[m][where], self.v[m][where], g)[0]
        else:
            self.scratch[0] = g
            for q in range(4):
                rows = pl.ds(12 * q, 12)
                where = (n, slice(None), pl.ds(512 * j + 128 * q, 128))
                self.scratch[1, rows, :] = adamw(
                    self.w[m][where].astype(F32), self.m[m][where], self.v[m][where], self.scratch[0, rows, :]
                )[0]
            new = self.scratch[1]
        self.full[m, j, x, y, z] = new.astype(BF16)

    def spread(self, m, c, phase, halves, k):
        axis, done = ORDER[c][2 - phase], ORDER[c][3 - phase :]
        where = tuple(slice(None) if a in done else k if a == axis else self.at[a] for a in range(3))
        return self.full.at[(m, halves, *where)]

    def gather_copies(self, m, c, phase, arriving=False):
        axis = ORDER[c][2 - phase]
        p, left, right = self.at[axis], self.left[axis], self.right[axis]
        both, a, b = pl.ds(2 * c, 2), pl.ds(2 * c, 1), pl.ds(2 * c + 1, 1)
        after, before, across = (p + 1) % 4, (p + 3) % 4, (p + 2) % 4
        parts = ((both, p, right), (both, p, left), (a, before, right), (b, after, left))
        if arriving:
            parts = ((both, before, right), (both, after, left), (a, across, right), (b, across, left))
        copies = []
        for i, (halves, k, to) in enumerate(parts):
            here = self.spread(m, c, phase, halves, k)
            copies.append(functools.partial(self.copy, (m, c, 3 + phase, i), here, here, to))
        return copies

    def out_copy(self, m, c):
        both = pl.ds(2 * c, 2)
        return pltpu.make_async_copy(self.full.at[m, both], self.out.at[m, both], self.out_sem.at[3 * m + c])

    def event(self, m, n):
        for c in range(3):
            if n == 0:
                self.begin(m, c, 0)
            elif n <= 6:
                phase = (n - 1) // 2
                if n % 2:
                    self.pass_on(m, c, phase)
                else:
                    self.finish(m, c, phase)
                    if phase < 2:
                        self.begin(m, c, phase + 1)
                    else:
                        for copy in self.gather_copies(m, c, 0)[:2]:
                            copy().start()
            else:
                phase = (n - 7) // 2
                copies = self.gather_copies(m, c, phase)
                arriving = self.gather_copies(m, c, phase, arriving=True)
                if n % 2:
                    for i in range(2):
                        arriving[i]().wait_recv()
                        copies[2 + i]().start()
                else:
                    arriving[2]().wait_recv()
                    arriving[3]().wait_recv()
                    if phase < 2:
                        for copy in self.gather_copies(m, c, phase + 1)[:2]:
                            copy().start()
                    else:
                        self.out_copy(m, c).start()

    def end(self):
        for m in range(3):
            for c in range(3):
                for phase in range(3):
                    for copy in self.reduce_copies(m, c, phase):
                        copy().wait_send()
                    for copy in self.gather_copies(m, c, phase):
                        copy().wait_send()
                self.out_copy(m, c).wait()


EVENTS = 13


def staggered(lag):
    order = []
    for t in range(EVENTS + 2 * lag):
        order += [(m, t - lag * m) for m in range(3) if 0 <= t - lag * m < EVENTS]
    return order


def exchange_kernel(number, *refs):
    g, w, m, v = (refs[i : i + 3] for i in (0, 3, 6, 9))
    sums, out = refs[12:14]
    full, own, scratch = refs[14:17]
    bufs = [refs[17 + 3 * i : 20 + 3 * i] for i in range(3)]
    sems = refs[26:30]
    ex = Exchange(number, g, w, m, v, sums, full, out, bufs, own, scratch, sems)
    ex.barrier()
    for event in staggered(1):
        ex.event(*event)
    ex.end()


def exchange(number, g, w, m, v):
    shapes = [(3, 3, 2, 4, 4, 48, 128), (3, 3, 2, 4, 48, 128), (3, 3, 2, 48, 128)]
    return pl.pallas_call(
        functools.partial(exchange_kernel, number),
        in_specs=[ANY] * 3 + [VMEM] * 9,
        out_specs=[VMEM, ANY],
        out_shape=[jax.ShapeDtypeStruct((3, 6, 48, 128), F32), jax.ShapeDtypeStruct((3, 6, 4, 4, 4, 48, 128), BF16)],
        scratch_shapes=[
            pltpu.VMEM((3, 6, 4, 4, 4, 48, 128), BF16),
            pltpu.VMEM((3, 3, 4, 4, 4, 48, 128), BF16),
            pltpu.VMEM((2, 48, 128), F32),
            *[pltpu.VMEM(s, BF16) for s in shapes for _ in range(3)],
            pltpu.SemaphoreType.DMA((9, 36)),
            pltpu.SemaphoreType.DMA((9, 36)),
            pltpu.SemaphoreType.DMA((9, 4)),
            pltpu.SemaphoreType.DMA((9,)),
        ],
        compiler_params=pltpu.CompilerParams(collective_id=number, has_side_effects=True, vmem_limit_bytes=VMEM_LIMIT),
        name=f"exchange_{number}",
    )(*[t.reshape(6, 4, 4, 4, 48, 128) for t in g], *w, *m, *v)


def results_kernel(*refs):
    full, sums, m, v = refs[0:2], refs[2:4], refs[4:7], refs[7:10]
    new_w, new_m, new_v = refs[10:13], refs[13:16], refs[16:19]
    for n in range(2):
        for j in range(6):
            columns = pl.ds(128 * j, 128)
            new_w[0][n, :, columns] = full[n][0, j].reshape(192, 128)
            for k in (1, 2):
                block = full[n][k, j].astype(F32)
                for q in range(4):
                    rows = jnp.concatenate([block[z, 12 * q : 12 * q + 12] for z in range(4)], axis=0)
                    new_w[k][n, :, pl.ds(512 * j + 128 * q, 128)] = rows.astype(BF16)

    @pl.when(pl.program_id(0) == 0)
    def _():
        for n in range(2):
            for j in range(6):
                for k in range(3):
                    for q in range(4 if k else 1):
                        g = sums[n][k, j, 12 * q : 12 * q + 12, :] if k else sums[n][k, j]
                        where = (n, slice(None), pl.ds(512 * j + 128 * q if k else 128 * j, 128))
                        new_m[k][where] = 0.9 * m[k][where] + 0.1 * g
                        new_v[k][where] = 0.95 * v[k][where] + 0.05 * g * g


def results(full, sums, m, v):
    def whole(t):
        return pl.BlockSpec(t.shape, lambda i: (0,) * t.ndim)

    full = [t.reshape(3, 6, 64, 48, 128) for t in full]
    part = pl.BlockSpec((3, 6, 4, 48, 128), lambda i: (0, 0, i, 0, 0))
    shapes = [(2, 3072, 768), (2, 768, 3072), (2, 768, 3072)]
    return pl.pallas_call(
        results_kernel,
        grid=(16,),
        in_specs=[part] * 2 + [whole(t) for t in (*sums, *m, *v)],
        out_specs=[pl.BlockSpec((2, s[1] // 16, s[2]), lambda i: (0, i, 0)) for s in shapes] + [whole(t) for t in (*m, *v)],
        out_shape=[jax.ShapeDtypeStruct(s, BF16) for s in shapes] + [jax.ShapeDtypeStruct(t.shape, F32) for t in (*m, *v)],
        compiler_params=pltpu.CompilerParams(vmem_limit_bytes=VMEM_LIMIT),
        name="results",
    )(*full, *sums, *m, *v)


def scale_of(wide):
    return lax.rsqrt(jnp.mean(wide**2, -1, keepdims=True) + 1e-6)


def normed(h):
    wide = h.astype(F32)
    return (wide * scale_of(wide)).astype(BF16)


def normed_back(h, d):
    wide, d = h.astype(F32), d.astype(F32)
    scale = scale_of(wide)
    return (scale * d - wide * (scale**3 * jnp.mean(wide * d, -1, keepdims=True))).astype(BF16)


def wide_of(a, w_gate, w_up):
    return jnp.dot(a, w_gate, preferred_element_type=F32), jnp.dot(a, w_up, preferred_element_type=F32)


def back_of_gate(gate, up, d):
    d = d.astype(F32)
    sig = jax.nn.sigmoid(gate)
    silu = gate * sig
    return (d * up * (sig + silu * (1 - sig))).astype(BF16), (d * silu).astype(BF16)


def solution(mesh):
    def step(x, dy, w_gate, w_up, w_down, m_gate, m_up, m_down, v_gate, v_up, v_down):
        h0, dy = x[0], dy[0]
        me = lax.axis_index("dp")
        w = (w_down, w_gate, w_up)
        m, v = (m_down, m_gate, m_up), (v_down, v_gate, v_up)
        mine = [lax.dynamic_slice_in_dim(t, me * (t.shape[1] // 64), t.shape[1] // 64, 1) for t in w]

        a0 = normed(h0)
        gate0, up0 = wide_of(a0, w_gate[0], w_up[0])
        act0 = (jax.nn.silu(gate0) * up0).astype(BF16)
        h1 = h0 + matmul(act0, w_down[0])
        a1 = normed(h1)
        gate1, up1 = wide_of(a1, w_gate[1], w_up[1])
        act1 = (jax.nn.silu(gate1) * up1).astype(BF16)

        d_gate, d_up = back_of_gate(gate1, up1, matmul(dy, w_down[1].T))
        g1 = [down_gradient(act1, dy), wide_gradient(a1, d_gate), wide_gradient(a1, d_up)]
        d_a = matmul(d_gate, w_gate[1].T) + matmul(d_up, w_up[1].T)
        d_h = dy + normed_back(h1, d_a)
        sums1, full1 = exchange(1, g1, mine, m, v)

        d_gate, d_up = back_of_gate(gate0, up0, matmul(d_h, w_down[0].T))
        g0 = [down_gradient(act0, d_h), wide_gradient(a0, d_gate), wide_gradient(a0, d_up)]
        sums0, full0 = exchange(0, g0, mine, m, v)

        new = results((full0, full1), (sums0, sums1), m, v)
        return tuple(new[3 * i + k] for i in range(3) for k in (1, 2, 0))

    rows = P(None, "dp", None)
    return jax.shard_map(
        step,
        mesh=mesh,
        in_specs=(P(("rep", "dp")),) * 2 + (P(),) * 3 + (rows,) * 6,
        out_specs=(P("rep"),) * 3 + (P("rep", "dp"),) * 6,
        check_vma=False,
    )
```

```python
import functools

import jax
import jax.numpy as jnp
from jax import lax
from jax.experimental import pallas as pl
from jax.experimental.pallas import tpu as pltpu
from jax.sharding import PartitionSpec as P

F32 = jnp.float32
BF16 = jnp.bfloat16
MESH = pl.DeviceIdType.MESH
ANY = pl.BlockSpec(memory_space=pl.ANY)
VMEM = pl.BlockSpec(memory_space=pltpu.VMEM)
STRIDE = (16, 4, 1)
ORDER = ((0, 1, 2), (1, 2, 0), (2, 0, 1))
VMEM_LIMIT = 60 * 1024 * 1024
ALL_VMEM = 67_043_328


def matmul(a, w):
    return jnp.dot(a, w, preferred_element_type=F32).astype(BF16)


def over_tokens(a, b):
    return lax.dot_general(a, b, (((0,), (0,)), ((), ())), preferred_element_type=F32)


def over_columns(a, b):
    return lax.dot_general(a, b, (((1,), (1,)), ((), ())), preferred_element_type=F32)


def scale_of(wide):
    return lax.rsqrt(jnp.mean(wide**2, -1, keepdims=True) + 1e-6)


def normed(h):
    wide = h.astype(F32)
    return (wide * scale_of(wide)).astype(BF16)


def normed_back(h, d):
    wide, d = h.astype(F32), d.astype(F32)
    scale = scale_of(wide)
    return (scale * d - wide * (scale**3 * jnp.mean(wide * d, -1, keepdims=True))).astype(BF16)


def adamw(w, m, v, g):
    m = 0.9 * m + 0.1 * g
    v = 0.95 * v + 0.05 * g * g
    step = m * lax.rsqrt(v + 1e-8) + 0.1 * w
    return w - 0.02 * step, m, v


def split(d):
    return lax.div(d, 16), lax.rem(lax.div(d, 4), 4), lax.rem(d, 4)


def axes(m, c):
    return ORDER[(m + c) % 3]


class Exchange:
    def __init__(self, layer, place, refs):
        self.layer = layer
        self.at, self.after, self.across, self.before, self.right, self.left = place
        self.g, self.w, self.m, self.v, self.sum, self.full, self.new, self.bufs, self.own, self.scratch = refs[:10]
        self.send_sem, self.recv_sem, self.own_sem, self.new_sem = refs[10:]

    def sem(self, m, c):
        return 3 * m + c

    def copy(self, m, c, n, src, dst, to):
        return pltpu.make_async_remote_copy(
            src_ref=src,
            dst_ref=dst,
            send_sem=self.send_sem.at[self.sem(m, c), n],
            recv_sem=self.recv_sem.at[self.sem(m, c), n],
            device_id={"dp": to},
            device_id_type=MESH,
        )

    def block(self, m, c, phase, half, k):
        axis = axes(m, c)[phase]
        place = sorted(axes(m, c)[phase:]).index(axis)
        where = (slice(None),) * place + (k,)
        if phase == 0:
            return self.g.at[(3 * self.layer + m, 2 * c + half, *where)]
        return self.bufs[phase - 1][1].at[(m, c, half, *where)]

    def reduce_copies(self, m, c, phase):
        axis = axes(m, c)[phase]
        p, left, right = self.at[axis], self.left[axis], self.right[axis]
        one, of_left, of_right = (b.at[m, c] for b in self.bufs[phase])
        after, before, across = self.after[axis], self.before[axis], self.across[axis]
        block = functools.partial(self.block, m, c, phase)
        parts = (
            (block(0, across), one.at[0], right),
            (block(1, across), one.at[1], left),
            (block(1, after), of_left.at[1], right),
            (block(0, before), of_right.at[0], left),
            (one.at[0], of_left.at[0], right),
            (one.at[1], of_right.at[1], left),
        )
        return [functools.partial(self.copy, m, c, 6 * phase + i, *part) for i, part in enumerate(parts)]

    def own_copies(self, m, c):
        axis = axes(m, c)[0]
        p = self.at[axis]
        blocks = ((0, self.after[axis]), (1, self.before[axis]), (0, p), (1, p))
        return [
            functools.partial(pltpu.make_async_copy, self.block(m, c, 0, *b), self.own.at[m, c, i % 2], self.own_sem.at[3 * m + c, i % 2])
            for i, b in enumerate(blocks)
        ]

    def add(self, phase, into, *others):
        def total(where):
            t = into[where].astype(F32)
            for o in others:
                t += o[where].astype(F32)
            into[where] = t.astype(BF16)

        if phase == 2:
            total(Ellipsis)
        elif phase == 1:
            for i in range(4):
                total((i,))
        else:

            def some(i, _):
                for k in range(4):
                    total((i, k))
                return 0

            lax.fori_loop(0, 4, some, 0)

    def begin(self, m, c, phase):
        for copy in self.reduce_copies(m, c, phase)[:4]:
            copy().start()
        if phase == 0:
            for copy in self.own_copies(m, c)[:2]:
                copy().start()

    def pass_on(self, m, c, phase):
        copies = self.reduce_copies(m, c, phase)
        axis = axes(m, c)[phase]
        one = self.bufs[phase][0].at[m, c]
        mine = self.own_copies(m, c) if phase == 0 else None
        for half, k in ((0, self.after[axis]), (1, self.before[axis])):
            if phase == 0:
                mine[half]().wait()
            copies[half]().wait_recv()
            self.add(phase, one.at[half], self.own.at[m, c, half] if phase == 0 else self.block(m, c, phase, half, k))
            copies[4 + half]().start()
            if phase == 0:
                mine[2 + half]().start()

    def finish(self, m, c, phase):
        copies = self.reduce_copies(m, c, phase)
        p = self.at[axes(m, c)[phase]]
        _, of_left, of_right = (b.at[m, c] for b in self.bufs[phase])
        mine = self.own_copies(m, c) if phase == 0 else None
        for half in range(2):
            if phase == 0:
                mine[2 + half]().wait()
            here = self.own.at[m, c, half] if phase == 0 else self.block(m, c, phase, half, p)
            for i in ((4, 3), (2, 5))[half]:
                copies[i]().wait_recv()
            if phase < 2:
                self.add(phase, of_left.at[half], of_right.at[half], here)
            else:
                self.update(m, 2 * c + half, of_left[half].astype(F32) + of_right[half].astype(F32) + here[...].astype(F32))

    def update(self, m, j, g):
        g = g.astype(BF16).astype(F32)
        n = self.layer
        self.sum[m, j] = g
        if m == 0:
            where = (n, slice(None), pl.ds(128 * j, 128))
            new = adamw(self.w[m][where].astype(F32), self.m[m][where], self.v[m][where], g)[0]
        else:
            self.scratch[0] = g
            for q in range(4):
                rows = pl.ds(12 * q, 12)
                where = (n, slice(None), pl.ds(512 * j + 128 * q, 128))
                self.scratch[1, rows, :] = adamw(
                    self.w[m][where].astype(F32), self.m[m][where], self.v[m][where], self.scratch[0, rows, :]
                )[0]
            new = self.scratch[1]
        self.new[m, j] = new.astype(BF16)

    def spread(self, m, c, phase, halves, k):
        axis, done = axes(m, c)[2 - phase], axes(m, c)[3 - phase :]
        where = tuple(slice(None) if a in done else k if a == axis else self.at[a] for a in range(3))
        return self.full.at[(m, halves, *where)]

    def gather_copies(self, m, c, phase, arriving=False):
        axis = axes(m, c)[2 - phase]
        p, left, right = self.at[axis], self.left[axis], self.right[axis]
        both, a, b = pl.ds(2 * c, 2), pl.ds(2 * c, 1), pl.ds(2 * c + 1, 1)
        after, before, across = self.after[axis], self.before[axis], self.across[axis]
        parts = ((both, p, right), (both, p, left), (a, before, right), (b, after, left))
        if arriving:
            parts = ((both, before, right), (both, after, left), (a, across, right), (b, across, left))
        copies = []
        for i, (halves, k, to) in enumerate(parts):
            here = self.spread(m, c, phase, halves, k)
            src = self.new.at[m, both] if phase == 0 and i < 2 else here
            copies.append(functools.partial(self.copy, m, c, 18 + 4 * phase + i, src, here, to))
        return copies

    def keep(self, m, c):
        x, y, z = self.at
        both = pl.ds(2 * c, 2)
        return pltpu.make_async_copy(
            self.new.at[m, both], self.full.at[m, both, x, y, z], self.new_sem.at[self.sem(m, c)]
        )

    def event(self, m, c, n):
        if n == 0:
            self.begin(m, c, 0)
        elif n <= 6:
            phase = (n - 1) // 2
            if n % 2:
                self.pass_on(m, c, phase)
            else:
                self.finish(m, c, phase)
                if phase < 2:
                    self.begin(m, c, phase + 1)
                else:
                    for copy in self.gather_copies(m, c, 0)[:2]:
                        copy().start()
                    self.keep(m, c).start()
        else:
            phase = (n - 7) // 2
            copies = self.gather_copies(m, c, phase)
            arriving = self.gather_copies(m, c, phase, arriving=True)
            if n % 2:
                for i in range(2):
                    arriving[i]().wait_recv()
                    copies[2 + i]().start()
            else:
                arriving[2]().wait_recv()
                arriving[3]().wait_recv()
                if n == 8:
                    self.keep(m, c).wait()
                if n == 10:
                    for i in range(3):
                        for copy in self.reduce_copies(m, c, i):
                            copy().wait_send()
                if phase < 2:
                    for copy in self.gather_copies(m, c, phase + 1)[:2]:
                        copy().start()

    def end(self):
        for m in range(3):
            for c in range(3):
                for phase in range(3):
                    for copy in self.gather_copies(m, c, phase):
                        copy().wait_send()


EVENTS = 13
UNITS, STEPS = 6, 7
TURN = UNITS * STEPS
LAST = 2 * TURN + 1
STEP_US = {1: (3.2,) * 4 + (2.7, 2.7, 2.5), 0: (2.2,) * 4 + (2.7, 2.7, 2.5)}
EVENT_US = (0.3, 0.8, 1.2, 0.3, 0.5, 0.2, 0.6, 0.2, 0.2, 0.2, 0.2, 0.2, 0.1)
HALF_US, HOP_US, SLACK_US = 4.3, 2.5, 1.0


def first_step(layer, m, c):
    if layer == 0:
        return 0
    return STEPS * (2 * c + 1) + 5 + m if m else TURN + 1


def schedule(layer, last):
    links = {}

    def send(time, axis, way, size):
        begin = max(time, links.get((axis, way), 0.0))
        links[axis, way] = begin + HALF_US * size
        return begin + HALF_US * size + HOP_US

    heads = {(layer, m, c): 0 for m in range(3) for c in range(3)}
    ready, forced = {}, {}
    order, now = [[] for _ in range(last + 1)], 0.0

    def run(key, time):
        layer, m, c = key
        n = heads[key]
        time += EVENT_US[n]
        heads[key] = n + 1
        arrival = time
        if n < 6:
            phase, size = n // 2, 0.25 ** (n // 2)
            axis = axes(m, c)[phase]
            if n % 2 == 0:
                forced[key] = 0.0
                for way in range(2):
                    arrival = max(arrival, send(time, axis, way, size))
                for way in range(2):
                    forced[key] = max(forced[key], send(time, axis, way, size))
            else:
                for way in range(2):
                    arrival = max(arrival, send(time, axis, way, size))
                arrival = max(arrival, forced[key])
        elif n < 12:
            phase, size = (n - 6) // 2, 0.25 ** (2 - (n - 6) // 2)
            axis = axes(m, c)[2 - phase]
            for way in range(2):
                arrival = max(arrival, send(time, axis, way, 2 * size if n % 2 == 0 else size))
        ready[key] = arrival
        return time

    for step in range(last + 1):
        while True:
            able = []
            for key, n in heads.items():
                if n == EVENTS:
                    continue
                if n == 0:
                    if step < first_step(*key):
                        continue
                    able.append((0.0, key))
                else:
                    able.append((ready[key] + SLACK_US, key))
            able.sort(key=lambda e: (e[0], -e[1][0], e[1][1:]))
            if not able or (step < last and able[0][0] > now):
                break
            time, key = able[0]
            order[step].append((*key, heads[key]))
            now = run(key, max(now, time))
        if step < last:
            now += 4.0 if step == TURN else STEP_US[1 if step < TURN else 0][(step - (step > TURN)) % STEPS]
    return order, now


def places():
    me = lax.axis_index("dp")
    at = split(me)
    after, across, before = (tuple(lax.rem(p + i, 4) for p in at) for i in (1, 2, 3))
    right, left = (tuple(me + STRIDE[i] * (to[i] - at[i]) for i in range(3)) for to in (after, before))
    return at, after, across, before, right, left


def greet(place):
    barrier = pltpu.get_barrier_semaphore()
    for axis in range(3):
        for to in (place[4][axis], place[5][axis]):
            pl.semaphore_signal(barrier, inc=1, device_id={"dp": to}, device_id_type=MESH)
    pl.semaphore_wait(barrier, 6)


def exchange_scratch():
    shapes = [(3, 3, 2, 4, 4, 48, 128), (3, 3, 2, 4, 48, 128), (3, 3, 2, 48, 128)]
    return [
        pltpu.VMEM((3, 3, 2, 4, 4, 48, 128), BF16),
        pltpu.VMEM((3, 6, 48, 128), BF16),
        pltpu.VMEM((2, 48, 128), F32),
        *[pltpu.VMEM(s, BF16) for s in shapes for _ in range(3)],
        pltpu.SemaphoreType.DMA((9, 30)),
        pltpu.SemaphoreType.DMA((9, 30)),
        pltpu.SemaphoreType.DMA((9, 2)),
        pltpu.SemaphoreType.DMA((9,)),
    ]


def exchange_of(layer, place, g, w, m, v, sums, full, scratch):
    own, new, small = scratch[:3]
    bufs = [scratch[3 + 3 * i : 6 + 3 * i] for i in range(3)]
    return Exchange(layer, place, (g, w, m, v, sums, full, new, bufs, own, small, *scratch[12:16]))


def exchange_kernel(*refs):
    g_ref = refs[0]
    w, m, v = refs[1:4], refs[4:7], refs[7:10]
    place = places()
    exchange = exchange_of(0, place, g_ref, w, m, v, *refs[10:12], refs[12:])
    greet(place)
    for _, m_, c, n in schedule(0, 0)[0][0]:
        exchange.event(m_, c, n)
    exchange.end()


EXCHANGED = [jax.ShapeDtypeStruct((3, 6, 48, 128), F32), jax.ShapeDtypeStruct((3, 6, 4, 4, 4, 48, 128), BF16)]


def exchange(g, w, m, v):
    return pl.pallas_call(
        exchange_kernel,
        in_specs=[ANY] + [VMEM] * 9,
        out_specs=[VMEM, ANY],
        out_shape=EXCHANGED,
        scratch_shapes=exchange_scratch(),
        compiler_params=pltpu.CompilerParams(collective_id=1, has_side_effects=True, vmem_limit_bytes=VMEM_LIMIT),
        name="exchange",
    )(g, *w, *m, *v)


def backward_kernel(*refs):
    a1_ref, a0_ref, h1_ref, dy_ref, w_gate_ref, w_up_ref, w_down_ref = refs[:7]
    w, m, v = refs[7:10], refs[10:13], refs[13:16]
    sum_ref, full_ref, g_ref = refs[16:19]
    a_ref, d_ref, da_ref, tile_ref, wg_ref, wu_ref, wd_ref, s_ref, wide_ref, down_ref, load_sem, weight_sem, store_sem = refs[19:32]
    place = places()
    exchange = exchange_of(1, place, g_ref, w, m, v, sum_ref, full_ref, refs[32:])

    def weights(unit):
        layer, j, slot = 1 - lax.div(unit, UNITS), lax.rem(unit, UNITS), lax.rem(unit, 2)
        some = pl.ds(pl.multiple_of(512 * j, 512), 512)
        return (
            pltpu.make_async_copy(w_gate_ref.at[layer, :, some], wg_ref.at[slot], weight_sem.at[slot, 0]),
            pltpu.make_async_copy(w_up_ref.at[layer, :, some], wu_ref.at[slot], weight_sem.at[slot, 1]),
            pltpu.make_async_copy(w_down_ref.at[layer, some, :], wd_ref.at[slot], weight_sem.at[slot, 2]),
        )

    def load(src, dst, i):
        return pltpu.make_async_copy(src, dst, load_sem.at[i])

    load(a1_ref, a_ref, 0).start()
    load(dy_ref, d_ref, 1).start()
    for copy in weights(jnp.int32(0)):
        copy.start()
    da_ref[...] = jnp.zeros_like(da_ref)
    load(a1_ref, a_ref, 0).wait()
    load(dy_ref, d_ref, 1).wait()
    greet(place)

    def tokens(layer, unit, block):
        rows = pl.ds(pl.multiple_of(512 * block, 512), 512)
        slot = lax.rem(unit, 2)
        a, d = a_ref[rows, :], d_ref[rows, :]
        gate = jnp.dot(a, wg_ref[slot], preferred_element_type=F32)
        up = jnp.dot(a, wu_ref[slot], preferred_element_type=F32)
        d_act = over_columns(d, wd_ref[slot]).astype(BF16).astype(F32)
        sig = jax.nn.sigmoid(gate)
        silu = gate * sig
        tile_ref[0, rows, :] = (silu * up).astype(BF16)
        d_gate = (d_act * up * (sig + silu * (1 - sig))).astype(BF16)
        d_up = (d_act * silu).astype(BF16)
        tile_ref[1, rows, :] = d_gate
        tile_ref[2, rows, :] = d_up

        @pl.when(layer == 1)
        def _():
            da_ref[rows, :] += over_columns(tile_ref[1, rows, :], wg_ref[slot]) + over_columns(tile_ref[2, rows, :], wu_ref[slot])

    def store_wide(layer, j, which):
        return pltpu.make_async_copy(wide_ref.at[which], g_ref.at[3 * layer + 1 + which, j], store_sem.at[which])

    def wide(layer, j, which):
        s_ref[...] = over_tokens(a_ref[...], tile_ref[1 + which])

        def two_devices(i, _):
            rows = s_ref[pl.ds(pl.multiple_of(24 * i, 8), 24), :]
            for k in range(2):
                block = [rows[12 * k : 12 * k + 12, 128 * q : 128 * q + 128] for q in range(4)]
                x, y, z = split(2 * i + k)
                wide_ref[which, x, y, z] = jnp.concatenate(block, axis=0).astype(BF16)
            return 0

        lax.fori_loop(0, 32, two_devices, 0)
        store_wide(layer, j, which).start()

        @pl.when(which == 1)
        def _():
            store_wide(layer, j, 0).wait()

    def store_down(layer):
        return pltpu.make_async_copy(down_ref, g_ref.at[3 * layer], store_sem.at[2])

    def down(layer, j):
        total = over_tokens(tile_ref[0], d_ref[...])
        for i in range(32):
            x, y, z = split(lax.div(32 * j + i, 3))
            rows = pl.ds(pl.multiple_of(16 * lax.rem(32 * j + i, 3), 16), 16)
            for k in range(6):
                down_ref[k, x, y, z, rows, :] = total[16 * i : 16 * i + 16, 128 * k : 128 * k + 128].astype(BF16)
        store_wide(layer, j, 1).wait()

        @pl.when(j == UNITS - 1)
        def _():
            store_down(layer).start()

    def turn():
        load(h1_ref, a_ref, 0).start()
        load(h1_ref, a_ref, 0).wait()

        def some(i, _):
            rows = pl.ds(pl.multiple_of(128 * i, 128), 128)
            back = normed_back(a_ref[rows, :], da_ref[rows, :].astype(BF16))
            d_ref[rows, :] = d_ref[rows, :] + back
            return 0

        lax.fori_loop(0, 16, some, 0)
        load(a0_ref, a_ref, 0).start()
        store_down(1).wait()
        load(a0_ref, a_ref, 0).wait()

    order, _ = schedule(1, LAST)

    def events(step, low, high):
        if not any(order[low:high]):
            return
        if high - low == 1:
            for _, m, c, n in order[low]:
                exchange.event(m, c, n)
            return
        middle = (low + high) // 2
        if any(order[low:middle]):
            pl.when(step < middle)(lambda: events(step, low, middle))
        if any(order[middle:high]):
            pl.when(step >= middle)(lambda: events(step, middle, high))

    def one_step(step, _):
        events(step, 0, LAST)
        turning = step == TURN
        at_work = jnp.where(step > TURN, step - 1, step)
        unit, kind = lax.div(at_work, STEPS), lax.rem(at_work, STEPS)
        layer, j = 1 - lax.div(unit, UNITS), lax.rem(unit, UNITS)
        working = jnp.logical_not(turning)

        @pl.when(jnp.logical_and(working, kind == 0))
        def _():
            for copy in weights(unit):
                copy.wait()

            @pl.when(unit < 2 * UNITS - 1)
            def _():
                for copy in weights(unit + 1):
                    copy.start()

        pl.when(jnp.logical_and(working, kind < 4))(lambda: tokens(layer, unit, kind))
        pl.when(jnp.logical_and(working, jnp.logical_or(kind == 4, kind == 5)))(lambda: wide(layer, j, kind - 4))
        pl.when(jnp.logical_and(working, kind == 6))(lambda: down(layer, j))
        pl.when(turning)(turn)
        return 0

    lax.fori_loop(0, LAST, one_step, 0)
    store_down(0).wait()
    for _, m_, c, n in order[LAST]:
        exchange.event(m_, c, n)
    exchange.end()


def backward(a1, a0, h1, dy, weights, w, m, v):
    tokens, d = a1.shape
    return pl.pallas_call(
        backward_kernel,
        in_specs=[ANY] * 7 + [VMEM] * 9,
        out_specs=[VMEM, ANY, ANY],
        out_shape=[*EXCHANGED, jax.ShapeDtypeStruct((6, 6, 4, 4, 4, 48, 128), BF16)],
        scratch_shapes=[
            pltpu.VMEM((tokens, d), BF16),
            pltpu.VMEM((tokens, d), BF16),
            pltpu.VMEM((tokens, d), F32),
            pltpu.VMEM((3, tokens, 512), BF16),
            pltpu.VMEM((2, d, 512), BF16),
            pltpu.VMEM((2, d, 512), BF16),
            pltpu.VMEM((2, 512, d), BF16),
            pltpu.VMEM((d, 512), F32),
            pltpu.VMEM((2, 4, 4, 4, 48, 128), BF16),
            pltpu.VMEM((6, 4, 4, 4, 48, 128), BF16),
            pltpu.SemaphoreType.DMA((2,)),
            pltpu.SemaphoreType.DMA((2, 3)),
            pltpu.SemaphoreType.DMA((3,)),
            *exchange_scratch(),
        ],
        compiler_params=pltpu.CompilerParams(collective_id=0, has_side_effects=True, vmem_limit_bytes=ALL_VMEM),
        name="backward",
    )(a1, a0, h1, dy, *weights, *w, *m, *v)


def results_kernel(*refs):
    full, sums, m, v = refs[0:2], refs[2:4], refs[4:7], refs[7:10]
    new_w, new_m, new_v = refs[10:13], refs[13:16], refs[16:19]
    for n in range(2):
        for j in range(6):
            columns = pl.ds(128 * j, 128)
            new_w[0][n, :, columns] = full[n][0, j].reshape(192, 128)
            for k in (1, 2):
                block = full[n][k, j].astype(F32)
                for q in range(4):
                    rows = jnp.concatenate([block[z, 12 * q : 12 * q + 12] for z in range(4)], axis=0)
                    new_w[k][n, :, pl.ds(512 * j + 128 * q, 128)] = rows.astype(BF16)

    @pl.when(pl.program_id(0) == 0)
    def _():
        for n in range(2):
            for j in range(6):
                for k in range(3):
                    for q in range(4 if k else 1):
                        g = sums[n][k, j, 12 * q : 12 * q + 12, :] if k else sums[n][k, j]
                        where = (n, slice(None), pl.ds(512 * j + 128 * q if k else 128 * j, 128))
                        new_m[k][where] = 0.9 * m[k][where] + 0.1 * g
                        new_v[k][where] = 0.95 * v[k][where] + 0.05 * g * g


def results(full, sums, m, v):
    def whole(t):
        return pl.BlockSpec(t.shape, lambda i: (0,) * t.ndim)

    full = [t.reshape(3, 6, 64, 48, 128) for t in full]
    part = pl.BlockSpec((3, 6, 4, 48, 128), lambda i: (0, 0, i, 0, 0))
    shapes = [(2, 3072, 768), (2, 768, 3072), (2, 768, 3072)]
    return pl.pallas_call(
        results_kernel,
        grid=(16,),
        in_specs=[part] * 2 + [whole(t) for t in (*sums, *m, *v)],
        out_specs=[pl.BlockSpec((2, s[1] // 16, s[2]), lambda i: (0, i, 0)) for s in shapes] + [whole(t) for t in (*m, *v)],
        out_shape=[jax.ShapeDtypeStruct(s, BF16) for s in shapes] + [jax.ShapeDtypeStruct(t.shape, F32) for t in (*m, *v)],
        compiler_params=pltpu.CompilerParams(vmem_limit_bytes=VMEM_LIMIT),
        name="results",
    )(*full, *sums, *m, *v)


def solution(mesh):
    def step(x, dy, w_gate, w_up, w_down, m_gate, m_up, m_down, v_gate, v_up, v_down):
        h0, dy = x[0], dy[0]
        me = lax.axis_index("dp")
        w = (w_down, w_gate, w_up)
        m, v = (m_down, m_gate, m_up), (v_down, v_gate, v_up)
        mine = [lax.dynamic_slice_in_dim(t, me * (t.shape[1] // 64), t.shape[1] // 64, 1) for t in w]

        a0 = normed(h0)
        gate = jnp.dot(a0, w_gate[0], preferred_element_type=F32)
        up = jnp.dot(a0, w_up[0], preferred_element_type=F32)
        h1 = h0 + matmul((jax.nn.silu(gate) * up).astype(BF16), w_down[0])
        a1 = normed(h1)
        sums1, full1, g = backward(a1, a0, h1, dy, (w_gate, w_up, w_down), mine, m, v)
        sums0, full0 = exchange(g, mine, m, v)
        new = results((full0, full1), (sums0, sums1), m, v)
        return tuple(new[3 * i + k] for i in range(3) for k in (1, 2, 0))

    rows = P(None, "dp", None)
    return jax.shard_map(
        step,
        mesh=mesh,
        in_specs=(P(("rep", "dp")),) * 2 + (P(),) * 3 + (rows,) * 6,
        out_specs=(P("rep"),) * 3 + (P("rep", "dp"),) * 6,
        check_vma=False,
    )
```

```python
import functools
import itertools

import jax
import jax.numpy as jnp
from jax import lax
from jax.experimental import pallas as pl
from jax.experimental.pallas import tpu as pltpu
from jax.sharding import PartitionSpec as P

F32 = jnp.float32
BF16 = jnp.bfloat16
MESH = pl.DeviceIdType.MESH
ANY = pl.BlockSpec(memory_space=pl.ANY)
VMEM = pl.BlockSpec(memory_space=pltpu.VMEM)
BLOCK = (48, 128)
CHIPS = (4, 4, 4)
STREAMS = 6
WIDE = 512
STRIDE = (16, 4, 1)
ORDER = tuple(tuple((i + k) % 3 for k in range(3)) for i in range(3))
VMEM_LIMIT = 60 * 1024 * 1024
ALL_VMEM = 67_043_328


def over_tokens(a, b):
    return lax.dot_general(a, b, (((0,), (0,)), ((), ())), preferred_element_type=F32)


def threes(refs):
    return [refs[i : i + 3] for i in range(0, len(refs), 3)]


def span(i, size):
    return slice(size * i, size * i + size)


def lanes(j):
    return pl.ds(128 * j, 128)


def quarter(j, q):
    return pl.ds(WIDE * j + 128 * q, 128)


def over_columns(a, b):
    return lax.dot_general(a, b, (((1,), (1,)), ((), ())), preferred_element_type=F32)


def scale_of(wide):
    return lax.rsqrt(jnp.mean(wide**2, -1, keepdims=True) + 1e-6)


def normed(h):
    wide = h.astype(F32)
    return (wide * scale_of(wide)).astype(BF16)


def normed_back(h, d):
    wide, d = h.astype(F32), d.astype(F32)
    scale = scale_of(wide)
    return (scale * d - wide * (scale**3 * jnp.mean(wide * d, -1, keepdims=True))).astype(BF16)


def adamw(w, m, v, g):
    m = 0.9 * m + 0.1 * g
    v = 0.95 * v + 0.05 * g * g
    step = m * lax.rsqrt(v + 1e-8) + 0.1 * w
    return w - 0.02 * step, m, v


def split(d):
    return lax.div(d, 16), lax.rem(lax.div(d, 4), 4), lax.rem(d, 4)


def axes(m, c):
    return ORDER[(m + c) % 3]


class Exchange:
    def __init__(self, layer, place, refs):
        self.layer = layer
        self.at, self.after, self.across, self.before, self.right, self.left = place
        self.g, self.w, self.m, self.v, self.sum, self.full, self.new, self.bufs, self.own, self.scratch = refs[:10]
        self.send_sem, self.recv_sem, self.own_sem, self.new_sem = refs[10:]

    def sem(self, m, c):
        return 3 * m + c

    def copy(self, m, c, n, src, dst, to):
        return pltpu.make_async_remote_copy(
            src_ref=src,
            dst_ref=dst,
            send_sem=self.send_sem.at[self.sem(m, c), n],
            recv_sem=self.recv_sem.at[self.sem(m, c), n],
            device_id={"dp": to},
            device_id_type=MESH,
        )

    def block(self, m, c, phase, half, k):
        axis = axes(m, c)[phase]
        place = sorted(axes(m, c)[phase:]).index(axis)
        where = (slice(None),) * place + (k,)
        if phase == 0:
            return self.g.at[(3 * self.layer + m, 2 * c + half, *where)]
        return self.bufs[phase - 1][1].at[(m, c, half, *where)]

    def reduce_copies(self, m, c, phase):
        axis = axes(m, c)[phase]
        p, left, right = self.at[axis], self.left[axis], self.right[axis]
        one, of_left, of_right = (b.at[m, c] for b in self.bufs[phase])
        after, before, across = self.after[axis], self.before[axis], self.across[axis]
        block = functools.partial(self.block, m, c, phase)
        parts = (
            (block(0, across), one.at[0], right),
            (block(1, across), one.at[1], left),
            (block(1, after), of_left.at[1], right),
            (block(0, before), of_right.at[0], left),
            (one.at[0], of_left.at[0], right),
            (one.at[1], of_right.at[1], left),
        )
        return [functools.partial(self.copy, m, c, 6 * phase + i, *part) for i, part in enumerate(parts)]

    def own_copies(self, m, c):
        axis = axes(m, c)[0]
        p = self.at[axis]
        blocks = ((0, self.after[axis]), (1, self.before[axis]), (0, p), (1, p))
        return [
            functools.partial(pltpu.make_async_copy, self.block(m, c, 0, *b), self.own.at[m, c, i % 2], self.own_sem.at[3 * m + c, i % 2])
            for i, b in enumerate(blocks)
        ]

    def add(self, phase, into, *others):
        def total(where):
            t = into[where].astype(F32)
            for o in others:
                t += o[where].astype(F32)
            into[where] = t.astype(BF16)

        if phase == 2:
            total(Ellipsis)
        elif phase == 1:
            for i in range(4):
                total((i,))
        else:

            def some(i, _):
                for k in range(4):
                    total((i, k))
                return 0

            lax.fori_loop(0, 4, some, 0)

    def begin(self, m, c, phase):
        for copy in self.reduce_copies(m, c, phase)[:4]:
            copy().start()
        if phase == 0:
            for copy in self.own_copies(m, c)[:2]:
                copy().start()

    def pass_on(self, m, c, phase):
        copies = self.reduce_copies(m, c, phase)
        axis = axes(m, c)[phase]
        one = self.bufs[phase][0].at[m, c]
        mine = self.own_copies(m, c) if phase == 0 else None
        for half, k in ((0, self.after[axis]), (1, self.before[axis])):
            if phase == 0:
                mine[half]().wait()
            copies[half]().wait_recv()
            self.add(phase, one.at[half], self.own.at[m, c, half] if phase == 0 else self.block(m, c, phase, half, k))
            copies[4 + half]().start()
            if phase == 0:
                mine[2 + half]().start()

    def finish(self, m, c, phase):
        copies = self.reduce_copies(m, c, phase)
        p = self.at[axes(m, c)[phase]]
        _, of_left, of_right = (b.at[m, c] for b in self.bufs[phase])
        mine = self.own_copies(m, c) if phase == 0 else None
        for half in range(2):
            if phase == 0:
                mine[2 + half]().wait()
            here = self.own.at[m, c, half] if phase == 0 else self.block(m, c, phase, half, p)
            for i in ((4, 3), (2, 5))[half]:
                copies[i]().wait_recv()
            if phase < 2:
                self.add(phase, of_left.at[half], of_right.at[half], here)
            else:
                self.update(m, 2 * c + half, of_left[half].astype(F32) + of_right[half].astype(F32) + here[...].astype(F32))

    def update(self, m, j, g):
        g = g.astype(BF16).astype(F32)
        n = self.layer
        self.sum[m, j] = g
        if m == 0:
            where = (n, slice(None), lanes(j))
            new = adamw(self.w[m][where].astype(F32), self.m[m][where], self.v[m][where], g)[0]
        else:
            self.scratch[0] = g
            for q in range(4):
                rows = span(q, 12)
                columns = quarter(j, q)
                self.scratch[1, rows, :] = adamw(
                    self.w[m][n, :, columns].astype(F32),
                    self.m[m][:, n, columns],
                    self.v[m][:, n, columns],
                    self.scratch[0, rows, :],
                )[0]
            new = self.scratch[1]
        self.new[m, j] = new.astype(BF16)

    def spread(self, m, c, phase, halves, k):
        axis, done = axes(m, c)[2 - phase], axes(m, c)[3 - phase :]
        where = tuple(slice(None) if a in done else k if a == axis else self.at[a] for a in range(3))
        return self.full.at[(m, halves, *where)]

    def gather_copies(self, m, c, phase, arriving=False):
        axis = axes(m, c)[2 - phase]
        p, left, right = self.at[axis], self.left[axis], self.right[axis]
        both, a, b = pl.ds(2 * c, 2), pl.ds(2 * c, 1), pl.ds(2 * c + 1, 1)
        after, before, across = self.after[axis], self.before[axis], self.across[axis]
        parts = ((both, p, right), (both, p, left), (a, before, right), (b, after, left))
        if arriving:
            parts = ((both, before, right), (both, after, left), (a, across, right), (b, across, left))
        copies = []
        for i, (halves, k, to) in enumerate(parts):
            here = self.spread(m, c, phase, halves, k)
            src = self.new.at[m, both] if phase == 0 and i < 2 else here
            copies.append(functools.partial(self.copy, m, c, 18 + 4 * phase + i, src, here, to))
        return copies

    def keep(self, m, c):
        x, y, z = self.at
        both = pl.ds(2 * c, 2)
        return pltpu.make_async_copy(
            self.new.at[m, both], self.full.at[m, both, x, y, z], self.new_sem.at[self.sem(m, c)]
        )

    def event(self, m, c, n):
        if n == 0:
            self.begin(m, c, 0)
        elif n <= 6:
            phase = (n - 1) // 2
            if n % 2:
                self.pass_on(m, c, phase)
            else:
                self.finish(m, c, phase)
                if phase < 2:
                    self.begin(m, c, phase + 1)
                else:
                    for copy in self.gather_copies(m, c, 0)[:2]:
                        copy().start()
                    self.keep(m, c).start()
        else:
            phase = (n - 7) // 2
            copies = self.gather_copies(m, c, phase)
            arriving = self.gather_copies(m, c, phase, arriving=True)
            if n % 2:
                for i in range(2):
                    arriving[i]().wait_recv()
                    copies[2 + i]().start()
            else:
                arriving[2]().wait_recv()
                arriving[3]().wait_recv()
                if n == 8:
                    self.keep(m, c).wait()
                if n == 10:
                    for i in range(3):
                        for copy in self.reduce_copies(m, c, i):
                            copy().wait_send()
                if phase < 2:
                    for copy in self.gather_copies(m, c, phase + 1)[:2]:
                        copy().start()

    def end(self):
        for m in range(3):
            for c in range(3):
                for phase in range(3):
                    for copy in self.gather_copies(m, c, phase):
                        copy().wait_send()


EVENTS = 13
UNITS, STEPS = 6, 7
TURN = UNITS * STEPS
LAST = 2 * TURN + 1
STEP_US, EVENT_US = (2.1, 2.6), 0.3
HALF_US, HOP_US, SLACK_US = 4.3, 2.5, 0.0


def first_step(layer, m, c):
    if layer == 0:
        return 0
    return STEPS * (2 * c + 1) + 5 + m if m else TURN + 1


def schedule(layer, last):
    links = {}

    def send(time, axis, way, size):
        begin = max(time, links.get((axis, way), 0.0))
        links[axis, way] = begin + HALF_US * size
        return begin + HALF_US * size + HOP_US

    heads = {(layer, m, c): 0 for m in range(3) for c in range(3)}
    ready, forced = {}, {}
    order, now = [[] for _ in range(last + 1)], 0.0

    def run(key, time):
        layer, m, c = key
        n = heads[key]
        time += EVENT_US
        heads[key] = n + 1
        arrival = time
        if n < 6:
            phase, size = n // 2, 0.25 ** (n // 2)
            axis = axes(m, c)[phase]
            if n % 2 == 0:
                forced[key] = 0.0
                for way in range(2):
                    arrival = max(arrival, send(time, axis, way, size))
                for way in range(2):
                    forced[key] = max(forced[key], send(time, axis, way, size))
            else:
                for way in range(2):
                    arrival = max(arrival, send(time, axis, way, size))
                arrival = max(arrival, forced[key])
        elif n < 12:
            phase, size = (n - 6) // 2, 0.25 ** (2 - (n - 6) // 2)
            axis = axes(m, c)[2 - phase]
            for way in range(2):
                arrival = max(arrival, send(time, axis, way, 2 * size if n % 2 == 0 else size))
        ready[key] = arrival
        return time

    for step in range(last + 1):
        while True:
            able = []
            for key, n in heads.items():
                if n == EVENTS:
                    continue
                if n == 0:
                    if step < first_step(*key):
                        continue
                    able.append((0.0, key))
                else:
                    able.append((ready[key] + SLACK_US, key))
            able.sort(key=lambda e: (e[0], -e[1][0], e[1][1:]))
            if not able or (step < last and able[0][0] > now):
                break
            time, key = able[0]
            order[step].append((*key, heads[key]))
            now = run(key, max(now, time))
        if step < last:
            now += STEP_US[step <= TURN]
    return order, now


def places():
    me = lax.axis_index("dp")
    at = split(me)
    after, across, before = (tuple(lax.rem(p + i, 4) for p in at) for i in (1, 2, 3))
    right, left = (tuple(me + STRIDE[i] * (to[i] - at[i]) for i in range(3)) for to in (after, before))
    return at, after, across, before, right, left


def greet(place):
    barrier = pltpu.get_barrier_semaphore()
    for axis in range(3):
        for to in (place[4][axis], place[5][axis]):
            pl.semaphore_signal(barrier, inc=1, device_id={"dp": to}, device_id_type=MESH)
    pl.semaphore_wait(barrier, 6)


def exchange_scratch():
    shapes = [(3, 3, 2, *CHIPS[i:], *BLOCK) for i in (1, 2, 3)]
    return [
        pltpu.VMEM(shapes[0], BF16),
        pltpu.VMEM((3, STREAMS, *BLOCK), BF16),
        pltpu.VMEM((2, *BLOCK), F32),
        *[pltpu.VMEM(s, BF16) for s in shapes for _ in range(3)],
        pltpu.SemaphoreType.DMA((9, 30)),
        pltpu.SemaphoreType.DMA((9, 30)),
        pltpu.SemaphoreType.DMA((9, 2)),
        pltpu.SemaphoreType.DMA((9,)),
    ]


def exchange_of(layer, place, g, w, m, v, sums, full, scratch):
    own, new, small = scratch[:3]
    return Exchange(layer, place, (g, w, m, v, sums, full, new, threes(scratch[3:12]), own, small, *scratch[12:]))


def exchange_kernel(*refs):
    g_ref, *refs = refs
    w, m, v = threes(refs[:9])
    place = places()
    exchange = exchange_of(0, place, g_ref, w, m, v, *refs[9:11], refs[11:])
    greet(place)
    for _, m_, c, n in schedule(0, 0)[0][0]:
        exchange.event(m_, c, n)
    exchange.end()


EXCHANGED = [jax.ShapeDtypeStruct((3, STREAMS, *BLOCK), F32), jax.ShapeDtypeStruct((3, STREAMS, *CHIPS, *BLOCK), BF16)]


def exchange(g, w, m, v):
    return pl.pallas_call(
        exchange_kernel,
        in_specs=[ANY] + [VMEM] * 9,
        out_specs=[VMEM, ANY],
        out_shape=EXCHANGED,
        scratch_shapes=exchange_scratch(),
        compiler_params=pltpu.CompilerParams(collective_id=1, has_side_effects=True, vmem_limit_bytes=VMEM_LIMIT),
        name="exchange",
    )(g, *w, *m, *v)


def backward_kernel(*refs):
    a1_ref, a0_ref, h1_ref, dy_ref, w_gate_ref, w_up_ref, w_down_ref = refs[:7]
    w, m, v = threes(refs[7:16])
    sum_ref, full_ref, g_ref = refs[16:19]
    a_ref, d_ref, da_ref, tile_ref, wg_ref, wu_ref, wd_ref, s_ref, wide_ref, down_ref, load_sem, weight_sem, store_sem = refs[19:32]
    place = places()
    exchange = exchange_of(1, place, g_ref, w, m, v, sum_ref, full_ref, refs[32:])

    def weights(unit):
        layer, j, slot = 1 - lax.div(unit, UNITS), lax.rem(unit, UNITS), lax.rem(unit, 2)
        some = pl.ds(pl.multiple_of(WIDE * j, WIDE), WIDE)
        return (
            pltpu.make_async_copy(w_gate_ref.at[layer, :, some], wg_ref.at[slot], weight_sem.at[slot, 0]),
            pltpu.make_async_copy(w_up_ref.at[layer, :, some], wu_ref.at[slot], weight_sem.at[slot, 1]),
            pltpu.make_async_copy(w_down_ref.at[layer, some, :], wd_ref.at[slot], weight_sem.at[slot, 2]),
        )

    def load(src, dst, i):
        return pltpu.make_async_copy(src, dst, load_sem.at[i])

    load(a1_ref, a_ref, 0).start()
    load(dy_ref, d_ref, 1).start()
    for copy in weights(jnp.int32(0)):
        copy.start()
    da_ref[...] = jnp.zeros_like(da_ref)
    load(a1_ref, a_ref, 0).wait()
    load(dy_ref, d_ref, 1).wait()
    greet(place)

    def tokens(layer, unit, block):
        rows = pl.ds(pl.multiple_of(WIDE * block, WIDE), WIDE)
        slot = lax.rem(unit, 2)
        a, d = a_ref[rows, :], d_ref[rows, :]
        gate = jnp.dot(a, wg_ref[slot], preferred_element_type=F32)
        up = jnp.dot(a, wu_ref[slot], preferred_element_type=F32)
        d_act = over_columns(d, wd_ref[slot]).astype(BF16).astype(F32)
        sig = jax.nn.sigmoid(gate)
        silu = gate * sig
        tile_ref[0, rows, :] = (silu * up).astype(BF16)
        d_gate = (d_act * up * (sig + silu * (1 - sig))).astype(BF16)
        d_up = (d_act * silu).astype(BF16)
        tile_ref[1, rows, :] = d_gate
        tile_ref[2, rows, :] = d_up

        @pl.when(layer == 1)
        def _():
            da_ref[rows, :] += over_columns(tile_ref[1, rows, :], wg_ref[slot]) + over_columns(tile_ref[2, rows, :], wu_ref[slot])

    def store_wide(layer, j, which):
        return pltpu.make_async_copy(wide_ref.at[which], g_ref.at[3 * layer + 1 + which, j], store_sem.at[which])

    def wide(layer, j, which):
        s_ref[...] = over_tokens(a_ref[...], tile_ref[1 + which])

        def two_devices(i, _):
            rows = s_ref[pl.ds(pl.multiple_of(24 * i, 8), 24), :]
            for k in range(2):
                block = [rows[span(k, 12), span(q, 128)] for q in range(4)]
                x, y, z = split(2 * i + k)
                wide_ref[which, x, y, z] = jnp.concatenate(block, axis=0).astype(BF16)
            return 0

        lax.fori_loop(0, 32, two_devices, 0)
        store_wide(layer, j, which).start()

        @pl.when(which == 1)
        def _():
            store_wide(layer, j, 0).wait()

    def store_down(layer):
        return pltpu.make_async_copy(down_ref, g_ref.at[3 * layer], store_sem.at[2])

    def down(layer, j):
        total = over_tokens(tile_ref[0], d_ref[...])
        for i in range(32):
            x, y, z = split(lax.div(32 * j + i, 3))
            rows = pl.ds(pl.multiple_of(16 * lax.rem(32 * j + i, 3), 16), 16)
            for k in range(6):
                down_ref[k, x, y, z, rows, :] = total[span(i, 16), span(k, 128)].astype(BF16)
        store_wide(layer, j, 1).wait()

        @pl.when(j == UNITS - 1)
        def _():
            store_down(layer).start()

    def turn():
        load(h1_ref, a_ref, 0).start()
        load(h1_ref, a_ref, 0).wait()

        def some(i, _):
            rows = pl.ds(pl.multiple_of(128 * i, 128), 128)
            back = normed_back(a_ref[rows, :], da_ref[rows, :].astype(BF16))
            d_ref[rows, :] = d_ref[rows, :] + back
            return 0

        lax.fori_loop(0, 16, some, 0)
        load(a0_ref, a_ref, 0).start()
        store_down(1).wait()
        load(a0_ref, a_ref, 0).wait()

    order, _ = schedule(1, LAST)

    def events(step, low, high):
        if not any(order[low:high]):
            return
        if high - low == 1:
            for _, m, c, n in order[low]:
                exchange.event(m, c, n)
            return
        middle = (low + high) // 2
        if any(order[low:middle]):
            pl.when(step < middle)(lambda: events(step, low, middle))
        if any(order[middle:high]):
            pl.when(step >= middle)(lambda: events(step, middle, high))

    def one_step(step, _):
        events(step, 0, LAST)
        turning = step == TURN
        at_work = jnp.where(step > TURN, step - 1, step)
        unit, kind = lax.div(at_work, STEPS), lax.rem(at_work, STEPS)
        layer, j = 1 - lax.div(unit, UNITS), lax.rem(unit, UNITS)
        working = jnp.logical_not(turning)

        @pl.when(jnp.logical_and(working, kind == 0))
        def _():
            for copy in weights(unit):
                copy.wait()

            @pl.when(unit < 2 * UNITS - 1)
            def _():
                for copy in weights(unit + 1):
                    copy.start()

        pl.when(jnp.logical_and(working, kind < 4))(lambda: tokens(layer, unit, kind))
        pl.when(jnp.logical_and(working, jnp.logical_or(kind == 4, kind == 5)))(lambda: wide(layer, j, kind - 4))
        pl.when(jnp.logical_and(working, kind == 6))(lambda: down(layer, j))
        pl.when(turning)(turn)
        return 0

    lax.fori_loop(0, LAST, one_step, 0)
    store_down(0).wait()
    for _, m_, c, n in order[LAST]:
        exchange.event(m_, c, n)
    exchange.end()


def backward(a1, a0, h1, dy, weights, w, m, v):
    tokens, d = a1.shape
    return pl.pallas_call(
        backward_kernel,
        in_specs=[ANY] * 7 + [VMEM] * 9,
        out_specs=[VMEM, ANY, ANY],
        out_shape=[*EXCHANGED, jax.ShapeDtypeStruct((6, STREAMS, *CHIPS, *BLOCK), BF16)],
        scratch_shapes=[
            pltpu.VMEM((tokens, d), BF16),
            pltpu.VMEM((tokens, d), BF16),
            pltpu.VMEM((tokens, d), F32),
            pltpu.VMEM((3, tokens, 512), BF16),
            pltpu.VMEM((2, d, 512), BF16),
            pltpu.VMEM((2, d, 512), BF16),
            pltpu.VMEM((2, 512, d), BF16),
            pltpu.VMEM((d, 512), F32),
            pltpu.VMEM((2, *CHIPS, *BLOCK), BF16),
            pltpu.VMEM((STREAMS, *CHIPS, *BLOCK), BF16),
            pltpu.SemaphoreType.DMA((2,)),
            pltpu.SemaphoreType.DMA((2, 3)),
            pltpu.SemaphoreType.DMA((3,)),
            *exchange_scratch(),
        ],
        compiler_params=pltpu.CompilerParams(collective_id=0, has_side_effects=True, vmem_limit_bytes=ALL_VMEM),
        name="backward",
    )(a1, a0, h1, dy, *weights, *w, *m, *v)


def results_kernel(*refs):
    full, sums = refs[:2], refs[2:4]
    m, v, new_w, new_m, new_v = threes(refs[4:])
    for n, part, j in itertools.product(range(2), range(2), range(6)):
        devices = span(part, 4)
        new_w[0][n, span(part, 192), lanes(j)] = full[n][0, j, devices].reshape(192, 128)
        for k in (1, 2):
            block = full[n][k, j, devices].astype(F32)
            for q in range(4):
                rows = jnp.concatenate([block[z, span(q, 12)] for z in range(4)], axis=0)
                new_w[k][n, span(part, 48), quarter(j, q)] = rows.astype(BF16)

    @pl.when(pl.program_id(0) == 0)
    def _():
        for n in range(2):
            for j in range(6):
                for k in range(3):
                    for q in range(4 if k else 1):
                        g = sums[n][k, j, span(q, 12), :] if k else sums[n][k, j]
                        where = (slice(None), n, quarter(j, q)) if k else (n, slice(None), lanes(j))
                        new_m[k][where] = 0.9 * m[k][where] + 0.1 * g
                        new_v[k][where] = 0.95 * v[k][where] + 0.05 * g * g


def results(full, sums, w, m, v):
    def whole(t):
        return pl.BlockSpec(t.shape, lambda i: (0,) * t.ndim)

    full = [t.reshape(3, STREAMS, 64, *BLOCK) for t in full]
    part = pl.BlockSpec((3, STREAMS, 8, *BLOCK), lambda i: (0, 0, i, 0, 0))
    shapes = [t.shape for t in w]
    return pl.pallas_call(
        results_kernel,
        grid=(8,),
        in_specs=[part] * 2 + [whole(t) for t in (*sums, *m, *v)],
        out_specs=[pl.BlockSpec((2, s[1] // 8, s[2]), lambda i: (0, i, 0)) for s in shapes] + [whole(t) for t in (*m, *v)],
        out_shape=[jax.ShapeDtypeStruct(s, BF16) for s in shapes] + [jax.ShapeDtypeStruct(t.shape, F32) for t in (*m, *v)],
        compiler_params=pltpu.CompilerParams(vmem_limit_bytes=VMEM_LIMIT),
        name="results",
    )(*full, *sums, *m, *v)


def forward_kernel(x_ref, w_gate_ref, w_up_ref, w_down_ref, a0_ref, h1_ref, a1_ref, total_ref):
    a0_ref[...] = normed(x_ref[0])
    total_ref[...] = jnp.zeros_like(total_ref)

    def unit(j, _):
        some = pl.ds(pl.multiple_of(WIDE * j, WIDE), WIDE)
        gate = jnp.dot(a0_ref[...], w_gate_ref[0, :, some], preferred_element_type=F32)
        up = jnp.dot(a0_ref[...], w_up_ref[0, :, some], preferred_element_type=F32)
        act = (jax.nn.silu(gate) * up).astype(BF16)
        total_ref[...] += jnp.dot(act, w_down_ref[0, some, :], preferred_element_type=F32)
        return 0

    lax.fori_loop(0, UNITS, unit, 0)
    h1 = x_ref[0] + total_ref[...].astype(BF16)
    h1_ref[...] = h1
    a1_ref[...] = normed(h1)


def forward(x, *weights):
    _, tokens, d = x.shape
    rows = pl.BlockSpec((WIDE, d), lambda i: (i, 0))
    return pl.pallas_call(
        forward_kernel,
        grid=(tokens // WIDE,),
        in_specs=[pl.BlockSpec((1, WIDE, d), lambda i: (0, i, 0))] + [pl.BlockSpec((1, *t.shape[1:]), lambda i: (0, 0, 0)) for t in weights],
        out_specs=[rows] * 3,
        out_shape=[jax.ShapeDtypeStruct((tokens, d), BF16)] * 3,
        scratch_shapes=[pltpu.VMEM((WIDE, d), F32)],
        compiler_params=pltpu.CompilerParams(vmem_limit_bytes=VMEM_LIMIT),
        name="forward",
    )(x, *weights)


def rows_first(t):
    return jnp.transpose(t, (1, 0, 2))


def solution(mesh):
    def step(x, dy, w_gate, w_up, w_down, m_gate, m_up, m_down, v_gate, v_up, v_down):
        dy = dy[0]
        me = lax.axis_index("dp")
        w = (w_down, w_gate, w_up)
        m, v = ((t[0], *(rows_first(o) for o in t[1:])) for t in ((m_down, m_gate, m_up), (v_down, v_gate, v_up)))
        mine = [lax.dynamic_slice_in_dim(t, me * (t.shape[1] // 64), t.shape[1] // 64, 1) for t in w]

        a0, h1, a1 = forward(x, w_gate, w_up, w_down)
        sums1, full1, g = backward(a1, a0, h1, dy, (w_gate, w_up, w_down), mine, m, v)
        sums0, full0 = exchange(g, mine, m, v)
        new = results((full0, full1), (sums0, sums1), w, m, v)
        return tuple(rows_first(new[3 * i + k]) if i and k else new[3 * i + k] for i in range(3) for k in (1, 2, 0))

    rows = P(None, "dp", None)
    return jax.shard_map(
        step,
        mesh=mesh,
        in_specs=(P(("rep", "dp")),) * 2 + (P(),) * 3 + (rows,) * 6,
        out_specs=(P("rep"),) * 3 + (P("rep", "dp"),) * 6,
        check_vma=False,
    )
```

```python
import functools
import itertools

import jax
import jax.numpy as jnp
from jax import lax
from jax.experimental import pallas as pl
from jax.experimental.pallas import tpu as pltpu
from jax.sharding import PartitionSpec as P

F32 = jnp.float32
BF16 = jnp.bfloat16
MESH = pl.DeviceIdType.MESH
ANY = pl.BlockSpec(memory_space=pl.ANY)
VMEM = pl.BlockSpec(memory_space=pltpu.VMEM)
BLOCK = (48, 128)
CHIPS = (4, 4, 4)
STREAMS = 6
WIDE = 512
STRIDE = (16, 4, 1)
ORDER = tuple(tuple((i + k) % 3 for k in range(3)) for i in range(3))
VMEM_LIMIT = 60 * 1024 * 1024
ALL_VMEM = 67_043_328


def over_tokens(a, b):
    return lax.dot_general(a, b, (((0,), (0,)), ((), ())), preferred_element_type=F32)


def threes(refs):
    return [refs[i : i + 3] for i in range(0, len(refs), 3)]


def span(i, size):
    return slice(size * i, size * i + size)


def lanes(j):
    return pl.ds(128 * j, 128)


def quarter(j, q):
    return pl.ds(WIDE * j + 128 * q, 128)


def over_columns(a, b):
    return lax.dot_general(a, b, (((1,), (1,)), ((), ())), preferred_element_type=F32)


def scale_of(wide):
    return lax.rsqrt(jnp.mean(wide**2, -1, keepdims=True) + 1e-6)


def normed(h):
    wide = h.astype(F32)
    return (wide * scale_of(wide)).astype(BF16)


def normed_back(h, d):
    wide, d = h.astype(F32), d.astype(F32)
    scale = scale_of(wide)
    return (scale * d - wide * (scale**3 * jnp.mean(wide * d, -1, keepdims=True))).astype(BF16)


def adamw(w, m, v, g):
    m = 0.9 * m + 0.1 * g
    v = 0.95 * v + 0.05 * g * g
    step = m * lax.rsqrt(v + 1e-8) + 0.1 * w
    return w - 0.02 * step, m, v


def split(d):
    return lax.div(d, 16), lax.rem(lax.div(d, 4), 4), lax.rem(d, 4)


def axes(m, c):
    return ORDER[(m + c) % 3]


class Exchange:
    def __init__(self, layer, place, refs):
        self.layer = layer
        self.at, self.after, self.across, self.before, self.right, self.left = place
        self.g, self.w, self.m, self.v, self.sum, self.full, self.new, self.bufs, self.own, self.scratch = refs[:10]
        self.send_sem, self.recv_sem, self.own_sem, self.new_sem = refs[10:]

    def sem(self, m, c):
        return 3 * m + c

    def copy(self, m, c, n, src, dst, to):
        return pltpu.make_async_remote_copy(
            src_ref=src,
            dst_ref=dst,
            send_sem=self.send_sem.at[self.sem(m, c), n],
            recv_sem=self.recv_sem.at[self.sem(m, c), n],
            device_id={"dp": to},
            device_id_type=MESH,
        )

    def block(self, m, c, phase, half, k):
        axis = axes(m, c)[phase]
        place = sorted(axes(m, c)[phase:]).index(axis)
        where = (slice(None),) * place + (k,)
        if phase == 0:
            return self.g.at[(3 * self.layer + m, 2 * c + half, *where)]
        return self.bufs[phase - 1][1].at[(m, c, half, *where)]

    def reduce_copies(self, m, c, phase):
        axis = axes(m, c)[phase]
        p, left, right = self.at[axis], self.left[axis], self.right[axis]
        one, of_left, of_right = (b.at[m, c] for b in self.bufs[phase])
        after, before, across = self.after[axis], self.before[axis], self.across[axis]
        block = functools.partial(self.block, m, c, phase)
        parts = (
            (block(0, across), one.at[0], right),
            (block(1, across), one.at[1], left),
            (block(1, after), of_left.at[1], right),
            (block(0, before), of_right.at[0], left),
            (one.at[0], of_left.at[0], right),
            (one.at[1], of_right.at[1], left),
        )
        return [functools.partial(self.copy, m, c, 6 * phase + i, *part) for i, part in enumerate(parts)]

    def own_copies(self, m, c):
        axis = axes(m, c)[0]
        p = self.at[axis]
        blocks = ((0, self.after[axis]), (1, self.before[axis]), (0, p), (1, p))
        return [
            functools.partial(pltpu.make_async_copy, self.block(m, c, 0, *b), self.own.at[m, c, i % 2], self.own_sem.at[3 * m + c, i % 2])
            for i, b in enumerate(blocks)
        ]

    def add(self, phase, into, *others):
        def total(where):
            t = into[where].astype(F32)
            for o in others:
                t += o[where].astype(F32)
            into[where] = t.astype(BF16)

        if phase == 2:
            total(Ellipsis)
        elif phase == 1:
            for i in range(4):
                total((i,))
        else:

            def some(i, _):
                for k in range(4):
                    total((i, k))
                return 0

            lax.fori_loop(0, 4, some, 0)

    def begin(self, m, c, phase):
        for copy in self.reduce_copies(m, c, phase)[:4]:
            copy().start()
        if phase == 0:
            for copy in self.own_copies(m, c)[:2]:
                copy().start()

    def pass_on(self, m, c, phase):
        copies = self.reduce_copies(m, c, phase)
        axis = axes(m, c)[phase]
        one = self.bufs[phase][0].at[m, c]
        mine = self.own_copies(m, c) if phase == 0 else None
        for half, k in ((0, self.after[axis]), (1, self.before[axis])):
            if phase == 0:
                mine[half]().wait()
            copies[half]().wait_recv()
            self.add(phase, one.at[half], self.own.at[m, c, half] if phase == 0 else self.block(m, c, phase, half, k))
            copies[4 + half]().start()
            if phase == 0:
                mine[2 + half]().start()

    def finish(self, m, c, phase):
        copies = self.reduce_copies(m, c, phase)
        p = self.at[axes(m, c)[phase]]
        _, of_left, of_right = (b.at[m, c] for b in self.bufs[phase])
        mine = self.own_copies(m, c) if phase == 0 else None
        for half in range(2):
            if phase == 0:
                mine[2 + half]().wait()
            here = self.own.at[m, c, half] if phase == 0 else self.block(m, c, phase, half, p)
            for i in ((4, 3), (2, 5))[half]:
                copies[i]().wait_recv()
            if phase < 2:
                self.add(phase, of_left.at[half], of_right.at[half], here)
            else:
                self.update(m, 2 * c + half, of_left[half].astype(F32) + of_right[half].astype(F32) + here[...].astype(F32))

    def update(self, m, j, g):
        g = g.astype(BF16).astype(F32)
        n = self.layer
        self.sum[m, j] = g
        if m == 0:
            where = (n, slice(None), lanes(j))
            new = adamw(self.w[m][where].astype(F32), self.m[m][where], self.v[m][where], g)[0]
        else:
            self.scratch[0] = g
            for q in range(4):
                rows = span(q, 12)
                columns = quarter(j, q)
                self.scratch[1, rows, :] = adamw(
                    self.w[m][n, :, columns].astype(F32),
                    self.m[m][:, n, columns],
                    self.v[m][:, n, columns],
                    self.scratch[0, rows, :],
                )[0]
            new = self.scratch[1]
        self.new[m, j] = new.astype(BF16)

    def spread(self, m, c, phase, halves, k):
        axis, done = axes(m, c)[2 - phase], axes(m, c)[3 - phase :]
        where = tuple(slice(None) if a in done else k if a == axis else self.at[a] for a in range(3))
        return self.full.at[(m, halves, *where)]

    def gather_copies(self, m, c, phase, arriving=False):
        axis = axes(m, c)[2 - phase]
        p, left, right = self.at[axis], self.left[axis], self.right[axis]
        both, a, b = pl.ds(2 * c, 2), pl.ds(2 * c, 1), pl.ds(2 * c + 1, 1)
        after, before, across = self.after[axis], self.before[axis], self.across[axis]
        parts = ((both, p, right), (both, p, left), (a, before, right), (b, after, left))
        if arriving:
            parts = ((both, before, right), (both, after, left), (a, across, right), (b, across, left))
        copies = []
        for i, (halves, k, to) in enumerate(parts):
            here = self.spread(m, c, phase, halves, k)
            src = self.new.at[m, both] if phase == 0 and i < 2 else here
            copies.append(functools.partial(self.copy, m, c, 18 + 4 * phase + i, src, here, to))
        return copies

    def keep(self, m, c):
        x, y, z = self.at
        both = pl.ds(2 * c, 2)
        return pltpu.make_async_copy(
            self.new.at[m, both], self.full.at[m, both, x, y, z], self.new_sem.at[self.sem(m, c)]
        )

    def event(self, m, c, n):
        if n == 0:
            self.begin(m, c, 0)
        elif n <= 6:
            phase = (n - 1) // 2
            if n % 2:
                self.pass_on(m, c, phase)
            else:
                self.finish(m, c, phase)
                if phase < 2:
                    self.begin(m, c, phase + 1)
                else:
                    for copy in self.gather_copies(m, c, 0)[:2]:
                        copy().start()
                    self.keep(m, c).start()
        else:
            phase = (n - 7) // 2
            copies = self.gather_copies(m, c, phase)
            arriving = self.gather_copies(m, c, phase, arriving=True)
            if n % 2:
                for i in range(2):
                    arriving[i]().wait_recv()
                    copies[2 + i]().start()
            else:
                arriving[2]().wait_recv()
                arriving[3]().wait_recv()
                if n == 8:
                    self.keep(m, c).wait()
                if n == 10:
                    for i in range(3):
                        for copy in self.reduce_copies(m, c, i):
                            copy().wait_send()
                if phase < 2:
                    for copy in self.gather_copies(m, c, phase + 1)[:2]:
                        copy().start()

    def end(self):
        for m in range(3):
            for c in range(3):
                for phase in range(3):
                    for copy in self.gather_copies(m, c, phase):
                        copy().wait_send()


EVENTS = 13
UNITS, STEPS = 6, 7
TURN = UNITS * STEPS
LAST = 2 * TURN + 1
STEP_US, EVENT_US = (2.1, 2.6), 0.3
HALF_US, HOP_US, SLACK_US = 4.3, 2.5, 0.0


def first_step(layer, m, c):
    if layer == 0:
        return 0
    return STEPS * (2 * c + 1) + 5 + m if m else TURN + 1


def schedule(layer, last):
    links = {}

    def send(time, axis, way, size):
        begin = max(time, links.get((axis, way), 0.0))
        links[axis, way] = begin + HALF_US * size
        return begin + HALF_US * size + HOP_US

    heads = {(layer, m, c): 0 for m in range(3) for c in range(3)}
    ready, forced = {}, {}
    order, now = [[] for _ in range(last + 1)], 0.0

    def run(key, time):
        layer, m, c = key
        n = heads[key]
        time += EVENT_US
        heads[key] = n + 1
        arrival = time
        if n < 6:
            phase, size = n // 2, 0.25 ** (n // 2)
            axis = axes(m, c)[phase]
            if n % 2 == 0:
                forced[key] = 0.0
                for way in range(2):
                    arrival = max(arrival, send(time, axis, way, size))
                for way in range(2):
                    forced[key] = max(forced[key], send(time, axis, way, size))
            else:
                for way in range(2):
                    arrival = max(arrival, send(time, axis, way, size))
                arrival = max(arrival, forced[key])
        elif n < 12:
            phase, size = (n - 6) // 2, 0.25 ** (2 - (n - 6) // 2)
            axis = axes(m, c)[2 - phase]
            for way in range(2):
                arrival = max(arrival, send(time, axis, way, 2 * size if n % 2 == 0 else size))
        ready[key] = arrival
        return time

    for step in range(last + 1):
        while True:
            able = []
            for key, n in heads.items():
                if n == EVENTS:
                    continue
                if n == 0:
                    if step < first_step(*key):
                        continue
                    able.append((0.0, key))
                else:
                    able.append((ready[key] + SLACK_US, key))
            able.sort(key=lambda e: (e[0], -e[1][0], e[1][1:]))
            if not able or (step < last and able[0][0] > now):
                break
            time, key = able[0]
            order[step].append((*key, heads[key]))
            now = run(key, max(now, time))
        if step < last:
            now += STEP_US[step <= TURN]
    return order, now


def places():
    me = lax.axis_index("dp")
    at = split(me)
    after, across, before = (tuple(lax.rem(p + i, 4) for p in at) for i in (1, 2, 3))
    right, left = (tuple(me + STRIDE[i] * (to[i] - at[i]) for i in range(3)) for to in (after, before))
    return at, after, across, before, right, left


def greet(place):
    barrier = pltpu.get_barrier_semaphore()
    for axis in range(3):
        for to in (place[4][axis], place[5][axis]):
            pl.semaphore_signal(barrier, inc=1, device_id={"dp": to}, device_id_type=MESH)
    pl.semaphore_wait(barrier, 6)


def exchange_scratch():
    shapes = [(3, 3, 2, *CHIPS[i:], *BLOCK) for i in (1, 2, 3)]
    return [
        pltpu.VMEM(shapes[0], BF16),
        pltpu.VMEM((3, STREAMS, *BLOCK), BF16),
        pltpu.VMEM((2, *BLOCK), F32),
        *[pltpu.VMEM(s, BF16) for s in shapes for _ in range(3)],
        pltpu.SemaphoreType.DMA((9, 30)),
        pltpu.SemaphoreType.DMA((9, 30)),
        pltpu.SemaphoreType.DMA((9, 2)),
        pltpu.SemaphoreType.DMA((9,)),
    ]


def exchange_of(layer, place, g, w, m, v, sums, full, scratch):
    own, new, small = scratch[:3]
    return Exchange(layer, place, (g, w, m, v, sums, full, new, threes(scratch[3:12]), own, small, *scratch[12:]))


def exchange_kernel(*refs):
    g_ref, *refs = refs
    w, m, v = threes(refs[:9])
    place = places()
    exchange = exchange_of(0, place, g_ref, w, m, v, *refs[9:11], refs[11:])
    greet(place)
    for _, m_, c, n in schedule(0, 0)[0][0]:
        exchange.event(m_, c, n)
    exchange.end()


EXCHANGED = [jax.ShapeDtypeStruct((3, STREAMS, *BLOCK), F32), jax.ShapeDtypeStruct((3, STREAMS, *CHIPS, *BLOCK), BF16)]


def exchange(g, w, m, v):
    return pl.pallas_call(
        exchange_kernel,
        in_specs=[ANY] + [VMEM] * 9,
        out_specs=[VMEM, ANY],
        out_shape=EXCHANGED,
        scratch_shapes=exchange_scratch(),
        compiler_params=pltpu.CompilerParams(collective_id=1, has_side_effects=True, vmem_limit_bytes=VMEM_LIMIT),
        name="exchange",
    )(g, *w, *m, *v)


def backward_kernel(*refs):
    a1_ref, a0_ref, h1_ref, dy_ref, w_gate_ref, w_up_ref, w_down_ref = refs[:7]
    w, m, v = threes(refs[7:16])
    sum_ref, full_ref, g_ref = refs[16:19]
    a_ref, d_ref, da_ref, tile_ref, wg_ref, wu_ref, wd_ref, s_ref, wide_ref, down_ref, load_sem, weight_sem, store_sem = refs[19:32]
    place = places()
    exchange = exchange_of(1, place, g_ref, w, m, v, sum_ref, full_ref, refs[32:])

    def weights(unit):
        layer, j, slot = 1 - lax.div(unit, UNITS), lax.rem(unit, UNITS), lax.rem(unit, 2)
        some = pl.ds(pl.multiple_of(WIDE * j, WIDE), WIDE)
        return (
            pltpu.make_async_copy(w_gate_ref.at[layer, :, some], wg_ref.at[slot], weight_sem.at[slot, 0]),
            pltpu.make_async_copy(w_up_ref.at[layer, :, some], wu_ref.at[slot], weight_sem.at[slot, 1]),
            pltpu.make_async_copy(w_down_ref.at[layer, some, :], wd_ref.at[slot], weight_sem.at[slot, 2]),
        )

    def load(src, dst, i):
        return pltpu.make_async_copy(src, dst, load_sem.at[i])

    load(a1_ref, a_ref, 0).start()
    load(dy_ref, d_ref, 1).start()
    for copy in weights(jnp.int32(0)):
        copy.start()
    da_ref[...] = jnp.zeros_like(da_ref)
    load(a1_ref, a_ref, 0).wait()
    load(dy_ref, d_ref, 1).wait()
    greet(place)

    def tokens(layer, unit, block):
        rows = pl.ds(pl.multiple_of(WIDE * block, WIDE), WIDE)
        slot = lax.rem(unit, 2)
        a, d = a_ref[rows, :], d_ref[rows, :]
        gate = jnp.dot(a, wg_ref[slot], preferred_element_type=F32)
        up = jnp.dot(a, wu_ref[slot], preferred_element_type=F32)
        d_act = over_columns(d, wd_ref[slot]).astype(BF16).astype(F32)
        sig = jax.nn.sigmoid(gate)
        silu = gate * sig
        tile_ref[0, rows, :] = (silu * up).astype(BF16)
        d_gate = (d_act * up * (sig + silu * (1 - sig))).astype(BF16)
        d_up = (d_act * silu).astype(BF16)
        tile_ref[1, rows, :] = d_gate
        tile_ref[2, rows, :] = d_up

        @pl.when(layer == 1)
        def _():
            da_ref[rows, :] += over_columns(tile_ref[1, rows, :], wg_ref[slot]) + over_columns(tile_ref[2, rows, :], wu_ref[slot])

    def store_wide(layer, j, which):
        return pltpu.make_async_copy(wide_ref.at[which], g_ref.at[3 * layer + 1 + which, j], store_sem.at[which])

    def wide(layer, j, which):
        halves = s_ref.shape[0] // 2
        for half in range(2):
            s_ref[span(half, halves), :] = over_tokens(a_ref[:, span(half, halves)], tile_ref[1 + which])
        for d in range(64):
            block = [s_ref[span(d, 12), span(q, 128)] for q in range(4)]
            wide_ref[which, d // 16, d // 4 % 4, d % 4] = jnp.concatenate(block, axis=0).astype(BF16)
        store_wide(layer, j, which).start()

        @pl.when(which == 1)
        def _():
            store_wide(layer, j, 0).wait()

    def store_down(layer):
        return pltpu.make_async_copy(down_ref, g_ref.at[3 * layer], store_sem.at[2])

    def down(layer, j):
        total = over_tokens(tile_ref[0], d_ref[...])
        for i in range(32):
            x, y, z = split(lax.div(32 * j + i, 3))
            rows = pl.ds(pl.multiple_of(16 * lax.rem(32 * j + i, 3), 16), 16)
            for k in range(6):
                down_ref[k, x, y, z, rows, :] = total[span(i, 16), span(k, 128)].astype(BF16)
        store_wide(layer, j, 1).wait()

        @pl.when(j == UNITS - 1)
        def _():
            store_down(layer).start()

    def turn():
        load(h1_ref, a_ref, 0).start()
        load(h1_ref, a_ref, 0).wait()

        def some(i, _):
            rows = pl.ds(pl.multiple_of(128 * i, 128), 128)
            back = normed_back(a_ref[rows, :], da_ref[rows, :].astype(BF16))
            d_ref[rows, :] = d_ref[rows, :] + back
            return 0

        lax.fori_loop(0, 16, some, 0)
        load(a0_ref, a_ref, 0).start()
        store_down(1).wait()
        load(a0_ref, a_ref, 0).wait()

    order, _ = schedule(1, LAST)

    def events(step, low, high):
        if not any(order[low:high]):
            return
        if high - low == 1:
            for _, m, c, n in order[low]:
                exchange.event(m, c, n)
            return
        middle = (low + high) // 2
        if any(order[low:middle]):
            pl.when(step < middle)(lambda: events(step, low, middle))
        if any(order[middle:high]):
            pl.when(step >= middle)(lambda: events(step, middle, high))

    def one_step(step, _):
        events(step, 0, LAST)
        turning = step == TURN
        at_work = jnp.where(step > TURN, step - 1, step)
        unit, kind = lax.div(at_work, STEPS), lax.rem(at_work, STEPS)
        layer, j = 1 - lax.div(unit, UNITS), lax.rem(unit, UNITS)
        working = jnp.logical_not(turning)

        @pl.when(jnp.logical_and(working, kind == 0))
        def _():
            for copy in weights(unit):
                copy.wait()

            @pl.when(unit < 2 * UNITS - 1)
            def _():
                for copy in weights(unit + 1):
                    copy.start()

        pl.when(jnp.logical_and(working, kind < 4))(lambda: tokens(layer, unit, kind))
        pl.when(jnp.logical_and(working, jnp.logical_or(kind == 4, kind == 5)))(lambda: wide(layer, j, kind - 4))
        pl.when(jnp.logical_and(working, kind == 6))(lambda: down(layer, j))
        pl.when(turning)(turn)
        return 0

    lax.fori_loop(0, LAST, one_step, 0)
    store_down(0).wait()
    for _, m_, c, n in order[LAST]:
        exchange.event(m_, c, n)
    exchange.end()


def backward(a1, a0, h1, dy, weights, w, m, v):
    tokens, d = a1.shape
    return pl.pallas_call(
        backward_kernel,
        in_specs=[ANY] * 7 + [VMEM] * 9,
        out_specs=[VMEM, ANY, ANY],
        out_shape=[*EXCHANGED, jax.ShapeDtypeStruct((6, STREAMS, *CHIPS, *BLOCK), BF16)],
        scratch_shapes=[
            pltpu.VMEM((tokens, d), BF16),
            pltpu.VMEM((tokens, d), BF16),
            pltpu.VMEM((tokens, d), F32),
            pltpu.VMEM((3, tokens, 512), BF16),
            pltpu.VMEM((2, d, 512), BF16),
            pltpu.VMEM((2, d, 512), BF16),
            pltpu.VMEM((2, 512, d), BF16),
            pltpu.VMEM((d, 512), F32),
            pltpu.VMEM((2, *CHIPS, *BLOCK), BF16),
            pltpu.VMEM((STREAMS, *CHIPS, *BLOCK), BF16),
            pltpu.SemaphoreType.DMA((2,)),
            pltpu.SemaphoreType.DMA((2, 3)),
            pltpu.SemaphoreType.DMA((3,)),
            *exchange_scratch(),
        ],
        compiler_params=pltpu.CompilerParams(collective_id=0, has_side_effects=True, vmem_limit_bytes=ALL_VMEM),
        name="backward",
    )(a1, a0, h1, dy, *weights, *w, *m, *v)


def results_kernel(*refs):
    full, sums = refs[:2], refs[2:4]
    m, v, new_w, new_m, new_v = threes(refs[4:])
    for n, part, j in itertools.product(range(2), range(2), range(6)):
        devices = span(part, 4)
        new_w[0][n, span(part, 192), lanes(j)] = full[n][0, j, devices].reshape(192, 128)
        for k in (1, 2):
            block = full[n][k, j, devices].astype(F32)
            for q in range(4):
                rows = jnp.concatenate([block[z, span(q, 12)] for z in range(4)], axis=0)
                new_w[k][n, span(part, 48), quarter(j, q)] = rows.astype(BF16)

    @pl.when(pl.program_id(0) == 0)
    def _():
        for n in range(2):
            for j in range(6):
                for k in range(3):
                    for q in range(4 if k else 1):
                        g = sums[n][k, j, span(q, 12), :] if k else sums[n][k, j]
                        where = (slice(None), n, quarter(j, q)) if k else (n, slice(None), lanes(j))
                        new_m[k][where] = 0.9 * m[k][where] + 0.1 * g
                        new_v[k][where] = 0.95 * v[k][where] + 0.05 * g * g


def results(full, sums, w, m, v):
    def whole(t):
        return pl.BlockSpec(t.shape, lambda i: (0,) * t.ndim)

    full = [t.reshape(3, STREAMS, 64, *BLOCK) for t in full]
    part = pl.BlockSpec((3, STREAMS, 8, *BLOCK), lambda i: (0, 0, i, 0, 0))
    shapes = [t.shape for t in w]
    return pl.pallas_call(
        results_kernel,
        grid=(8,),
        in_specs=[part] * 2 + [whole(t) for t in (*sums, *m, *v)],
        out_specs=[pl.BlockSpec((2, s[1] // 8, s[2]), lambda i: (0, i, 0)) for s in shapes] + [whole(t) for t in (*m, *v)],
        out_shape=[jax.ShapeDtypeStruct(s, BF16) for s in shapes] + [jax.ShapeDtypeStruct(t.shape, F32) for t in (*m, *v)],
        compiler_params=pltpu.CompilerParams(vmem_limit_bytes=VMEM_LIMIT),
        name="results",
    )(*full, *sums, *m, *v)


def forward_kernel(x_ref, w_gate_ref, w_up_ref, w_down_ref, a0_ref, h1_ref, a1_ref, total_ref):
    a0_ref[...] = normed(x_ref[0])
    total_ref[...] = jnp.zeros_like(total_ref)

    def unit(j, _):
        some = pl.ds(pl.multiple_of(WIDE * j, WIDE), WIDE)
        gate = jnp.dot(a0_ref[...], w_gate_ref[0, :, some], preferred_element_type=F32)
        up = jnp.dot(a0_ref[...], w_up_ref[0, :, some], preferred_element_type=F32)
        act = (jax.nn.silu(gate) * up).astype(BF16)
        total_ref[...] += jnp.dot(act, w_down_ref[0, some, :], preferred_element_type=F32)
        return 0

    lax.fori_loop(0, UNITS, unit, 0, unroll=2)
    h1 = x_ref[0] + total_ref[...].astype(BF16)
    h1_ref[...] = h1
    a1_ref[...] = normed(h1)


def forward(x, *weights):
    _, tokens, d = x.shape
    rows = pl.BlockSpec((WIDE, d), lambda i: (i, 0))
    return pl.pallas_call(
        forward_kernel,
        grid=(tokens // WIDE,),
        in_specs=[pl.BlockSpec((1, WIDE, d), lambda i: (0, i, 0))] + [pl.BlockSpec((1, *t.shape[1:]), lambda i: (0, 0, 0)) for t in weights],
        out_specs=[rows] * 3,
        out_shape=[jax.ShapeDtypeStruct((tokens, d), BF16)] * 3,
        scratch_shapes=[pltpu.VMEM((WIDE, d), F32)],
        compiler_params=pltpu.CompilerParams(vmem_limit_bytes=VMEM_LIMIT),
        name="forward",
    )(x, *weights)


def rows_first(t):
    return jnp.transpose(t, (1, 0, 2))


def solution(mesh):
    def step(x, dy, w_gate, w_up, w_down, m_gate, m_up, m_down, v_gate, v_up, v_down):
        dy = dy[0]
        me = lax.axis_index("dp")
        w = (w_down, w_gate, w_up)
        m, v = ((t[0], *(rows_first(o) for o in t[1:])) for t in ((m_down, m_gate, m_up), (v_down, v_gate, v_up)))
        mine = [lax.dynamic_slice_in_dim(t, me * (t.shape[1] // 64), t.shape[1] // 64, 1) for t in w]

        a0, h1, a1 = forward(x, w_gate, w_up, w_down)
        sums1, full1, g = backward(a1, a0, h1, dy, (w_gate, w_up, w_down), mine, m, v)
        sums0, full0 = exchange(g, mine, m, v)
        new = results((full0, full1), (sums0, sums1), w, m, v)
        return tuple(rows_first(new[3 * i + k]) if i and k else new[3 * i + k] for i in range(3) for k in (1, 2, 0))

    rows = P(None, "dp", None)
    return jax.shard_map(
        step,
        mesh=mesh,
        in_specs=(P(("rep", "dp")),) * 2 + (P(),) * 3 + (rows,) * 6,
        out_specs=(P("rep"),) * 3 + (P("rep", "dp"),) * 6,
        check_vma=False,
    )
```
